16 devices in a mesh: dp: 2 (over z), tp: 8 (over y, x, core).
Axes of the slice: x: 2, y: 2, z: 2, core: 2. Of those that a mesh axis runs over, the one named last changes fastest.
Arguments:
- y1: float32 [4, 12, 64, 1664], P('dp'), parts along dimension 0
- y2: float32 [4, 12, 64, 1664], P('dp'), parts along dimension 0
- dy1: float32 [4, 12, 64, 1664], P('dp'), parts along dimension 0
- dy2: float32 [4, 12, 64, 1664], P('dp'), parts along dimension 0
- w_qkv: bfloat16 [3, 1664, 3, 16, 104], P(None, None, None, 'tp')
- w_out: bfloat16 [3, 16, 104, 1664], P(None, 'tp')
- w_up: bfloat16 [3, 1664, 8192], P(None, None, 'tp')
- w_down: bfloat16 [3, 8192, 1664], P(None, 'tp')
Outputs:
- output 1: float32 [4, 12, 64, 1664], P('dp'), parts along dimension 0
- output 2: float32 [4, 12, 64, 1664], P('dp'), parts along dimension 0
- output 3: float32 [4, 12, 64, 1664], P('dp'), parts along dimension 0
- output 4: float32 [4, 12, 64, 1664], P('dp'), parts along dimension 0
- output 5: float32 [6, 1664, 3, 16, 104], P('dp', None, None, 'tp'), parts along dimension 0
- output 6: float32 [6, 16, 104, 1664], P('dp', 'tp'), parts along dimension 0
- output 7: float32 [6, 1664, 8192], P('dp', None, 'tp'), parts along dimension 0
- output 8: float32 [6, 8192, 1664], P('dp', 'tp'), parts along dimension 0
There are 2 independent parts. The reference program is written for one: setup_inputs(seed, part) draws one part's arguments, and reference() takes and returns one part's arrays. A program takes and returns all parts, laid end to end along the dimension named above; an argument that names none is the same for every part.
All inputs are finite; a program needn't handle non-finite values.
Results may differ from the reference program's by a relative error of at most 0.0111879.
Values are sent between devices in bfloat16 or wider.
A program may use at most 1 GiB of HBM per device.

```python
import jax
import jax.numpy as jnp
from jax import lax

H = 1664
HEADS = 16
FF = 8192
BATCH = 12
SEQ = 64
LAYERS = 3
HEAD_DIM = H // HEADS
EPS = 1e-6


def setup_inputs(seed: int = 0, part: int = 0) -> dict:
    part_key = jax.random.fold_in(jax.random.key(seed), part)
    key_tok, key_seq, key_grad = jax.random.split(part_key, 3)
    act_shape = (2, 2, BATCH, SEQ, H)
    tok_noise = jax.random.normal(key_tok, act_shape, jnp.float32)
    seq_shared = jax.random.normal(key_seq, (2, 2, BATCH, 1, H), jnp.float32)
    y_pair = 0.8 * tok_noise + 0.6 * seq_shared
    dy_pair = jax.random.normal(key_grad, act_shape, jnp.float32)
    key_qkv, key_out, key_up, key_down = jax.random.split(jax.random.key(seed + 1), 4)
    branch_gain = (LAYERS + 2) ** -0.5
    w_qkv = jax.random.normal(key_qkv, (LAYERS, H, 3, HEADS, HEAD_DIM), jnp.float32) * H ** -0.5
    w_out = jax.random.normal(key_out, (LAYERS, HEADS, HEAD_DIM, H), jnp.float32) * (branch_gain * H ** -0.5)
    w_up = jax.random.normal(key_up, (LAYERS, H, FF), jnp.float32) * H ** -0.5
    w_down = jax.random.normal(key_down, (LAYERS, FF, H), jnp.float32) * (branch_gain * FF ** -0.5)
    return {'y1': y_pair[0], 'y2': y_pair[1], 'dy1': dy_pair[0], 'dy2': dy_pair[1],
            'w_qkv': w_qkv.astype(jnp.bfloat16), 'w_out': w_out.astype(jnp.bfloat16),
            'w_up': w_up.astype(jnp.bfloat16), 'w_down': w_down.astype(jnp.bfloat16)}


def to_bf16(value):
    return value.astype(jnp.bfloat16).astype(jnp.float32)


def rms_norm(x_in):
    return x_in * lax.rsqrt(jnp.mean(x_in * x_in, axis=-1, keepdims=True) + EPS)


def attend_one(qkv_seq):
    scores = jnp.einsum('qnd,knd->nqk', qkv_seq[0], qkv_seq[1]) * HEAD_DIM ** -0.5
    prob_half = to_bf16(jax.nn.softmax(scores, axis=-1))
    return to_bf16(jnp.einsum('nqk,knd->qnd', prob_half, qkv_seq[2]))


def branch_f(x_in, w_qkv, w_out):
    normed = to_bf16(rms_norm(x_in))
    qkv_all = to_bf16(jnp.einsum('rsh,hcnd->rcsnd', normed, w_qkv))
    attn_out = lax.map(jax.checkpoint(attend_one), qkv_all)
    return jnp.einsum('rsnd,ndh->rsh', attn_out, w_out)


def branch_g(x_in, w_up, w_down):
    normed = to_bf16(rms_norm(x_in))
    act_half = to_bf16(jax.nn.gelu(jnp.einsum('rsh,hf->rsf', normed, w_up)))
    return jnp.einsum('rsf,fh->rsh', act_half, w_down)


def reference(y1, y2, dy1, dy2, w_qkv, w_out, w_up, w_down):
    row_shape = (2 * BATCH, SEQ, H)

    def block_step(carry, weights):
        upper_one, upper_two, grad_one, grad_two = carry
        layer_qkv, layer_out, layer_up, layer_down = [weight.astype(jnp.float32) for weight in weights]
        g_val, g_pull = jax.vjp(branch_g, upper_one, layer_up, layer_down)
        lower_two = upper_two - g_val
        g_in, g_up, g_down = g_pull(grad_two)
        grad_one = grad_one + g_in
        f_val, f_pull = jax.vjp(branch_f, lower_two, layer_qkv, layer_out)
        lower_one = upper_one - f_val
        f_in, f_qkv, f_out = f_pull(grad_one)
        return (lower_one, lower_two, grad_one, grad_two + f_in), (f_qkv, f_out, g_up, g_down)

    start_carry = (y1.reshape(row_shape), y2.reshape(row_shape), dy1.reshape(row_shape), dy2.reshape(row_shape))
    layer_weights = (w_qkv[::-1], w_out[::-1], w_up[::-1], w_down[::-1])
    final_carry, grad_stack = lax.scan(block_step, start_carry, layer_weights)
    out_shape = (2, BATCH, SEQ, H)
    return (final_carry[0].reshape(out_shape), final_carry[1].reshape(out_shape),
            final_carry[2].reshape(out_shape), final_carry[3].reshape(out_shape),
            grad_stack[0][::-1], grad_stack[1][::-1], grad_stack[2][::-1], grad_stack[3][::-1])
```

```python
import functools

import jax
import jax.numpy as jnp
from jax import lax
from jax.experimental import pallas as pl
from jax.experimental.pallas import tpu as pltpu
from jax.sharding import PartitionSpec as P

EPS = 1e-6
BF = jnp.bfloat16
F32 = jnp.float32
GROUP = 8
CUT = 896
GELU_K = 0.7978845608028654
MESH = pl.DeviceIdType.MESH
VMEM_LIMIT = 67043328


def rms_norm(x_in):
    return x_in * lax.rsqrt(jnp.mean(x_in * x_in, axis=-1, keepdims=True) + EPS)


def dot(a, b, ca, cb):
    return lax.dot_general(a, b, (((ca,), (cb,)), ((), ())), preferred_element_type=F32)


def tiles(total, size, body):
    def step(i, carry):
        body(pl.multiple_of(i * size, size), size)
        return carry
    lax.fori_loop(0, total // size, step, 0)
    if total % size:
        body(total // size * size, total % size)


def half_block(kind, last, chunks, seq, heads, scale, *refs):
    (n_hbm, g_hbm, w1_hbm, w2_hbm, base_hbm, res_hbm, cot_hbm,
     next_n, next_g, res_out, cot_out, hid_out, dhid_out,
     n_buf, g_buf, w1, w2, own, hid, dhid, aux, s32, k32, r32, x32, y32, s16, k16, r16, x16, y16,
     quad_n, quad_g, qkv, d_att, in_sem, out_sem, send_sem, recv_sem) = refs
    if last:
        quad_n, quad_g = s32, r32
    width = n_buf.shape[-1]
    rows = GROUP * seq
    half = rows // 2
    me = lax.axis_index('tp')
    core, xax, yax = ({'tp': me + bit - 2 * bit * lax.rem(lax.div(me, bit), 2)} for bit in (1, 2, 4))

    barrier = pltpu.get_barrier_semaphore()
    for dev in (core, xax, yax):
        pl.semaphore_signal(barrier, inc=1, device_id=dev, device_id_type=MESH)

    loads = {}

    def load(name, src, dst, i):
        loads[name] = pltpu.make_async_copy(src, dst, in_sem.at[i])
        loads[name].start()

    load('w1', w1_hbm, w1, 0)
    for k in range(chunks):
        load(('n', k), n_hbm.at[pl.ds(k * rows, rows)], n_buf.at[k], 2 + 5 * k)
        if k == 0:
            load('w2', w2_hbm, w2, 1)
        load(('g', k), g_hbm.at[pl.ds(k * rows, rows)], g_buf.at[k], 3 + 5 * k)
    for k in range(chunks):
        for j, src in enumerate((base_hbm, res_hbm, cot_hbm)):
            load(('own', j, k), src.at[k], own.at[j, k], 4 + 5 * k + j)
    pl.semaphore_wait(barrier, 3)

    sent = []
    saved = []
    done = set()

    def remote(k, i, src, dst, dev):
        copy = pltpu.make_async_remote_copy(src_ref=src, dst_ref=dst, send_sem=send_sem.at[k, i],
                                            recv_sem=recv_sem.at[k, i], device_id=dev, device_id_type=MESH)
        copy.start()
        sent.append(copy)
        return copy

    def save(k, i, src, dst):
        copy = pltpu.make_async_copy(src, dst, out_sem.at[k, i])
        copy.start()
        saved.append(copy)
        return copy

    cols_a, cols_b = pl.ds(0, CUT), pl.ds(CUT, width - CUT)
    flight = {}
    slot_free = {}

    def blocks(v):
        return v.reshape(2, 2, seq, v.shape[-1])

    def send_partial(k, lhs, w, cw, s_ref, k_ref, name, i):
        def make(out, part):
            def tile(off, size):
                a = lhs[part * half:(part + 1) * half, :]
                b = w[:, pl.ds(off, size)] if cw == 0 else w[pl.ds(off, size), :]
                out[k, :, :, :, pl.ds(off, size)] = blocks(dot(a, b, 1, cw).astype(out.dtype))
            tiles(width, 256, tile)
        make(s_ref, 1)
        recv = r32 if name == 'f' else r16
        flight[name, k] = [remote(k, i, s_ref.at[k], recv.at[k], core)]
        make(k_ref, 0)

    def forward(k):
        slot = k % 2
        if k == 0:
            loads['w1'].wait()
        loads['n', k].wait()
        if k >= 2:
            for copy in slot_free[k - 2]:
                copy.wait()
                done.add(id(copy))
        if kind == 'mlp':
            def tile(off, size):
                u = dot(n_buf[k], w1[:, pl.ds(off, size)], 1, 0)
                t = jnp.tanh(GELU_K * (u + 0.044715 * u * u * u))
                hid[slot, :, pl.ds(off, size)] = (0.5 * u * (1.0 + t)).astype(BF)
                aux[:, pl.ds(off, size)] = 0.5 * (1.0 + t) + 0.5 * u * (1.0 - t * t) * (
                    GELU_K * (1.0 + 3 * 0.044715 * u * u))
            tiles(hid.shape[-1], 256, tile)
        else:
            def tile(off, size):
                qkv[:, pl.ds(off, size)] = dot(n_buf[k], w1[:, pl.ds(off, size)], 1, 0).astype(BF)
            tiles(qkv.shape[-1], 256, tile)
            dim = qkv.shape[-1] // (3 * heads)

            def one_seq(s, carry):
                r = pl.ds(pl.multiple_of(s * seq, seq), seq)
                for h in range(heads):
                    q = qkv[r, h * dim:(h + 1) * dim]
                    key = qkv[r, (heads + h) * dim:(heads + h + 1) * dim]
                    v = qkv[r, (2 * heads + h) * dim:(2 * heads + h + 1) * dim]
                    scores = dot(q, key, 1, 1) * scale
                    expd = jnp.exp(scores - jnp.max(scores, axis=-1, keepdims=True))
                    prob = expd / jnp.sum(expd, axis=-1, keepdims=True)
                    aux[r, h * seq:(h + 1) * seq] = prob
                    hid[slot, r, h * dim:(h + 1) * dim] = dot(prob.astype(BF), v, 1, 0).astype(BF)
                return carry
            lax.fori_loop(0, GROUP, one_seq, 0, unroll=4)
        first = save(k, 0, hid.at[slot], hid_out.at[pl.ds(k * rows, rows)])
        slot_free[k] = [first]
        if k == 0:
            loads['w2'].wait()
        send_partial(k, hid.at[slot], w2, 0, s32, k32, 'f', 0)

    def backward(k):
        slot = k % 2
        loads['g', k].wait()
        if kind == 'mlp':
            def tile(off, size):
                d_act = dot(g_buf[k], w2[pl.ds(off, size), :], 1, 1)
                dhid[slot, :, pl.ds(off, size)] = (d_act * aux[:, pl.ds(off, size)]).astype(BF)
            tiles(dhid.shape[-1], 256, tile)
        else:
            dim = qkv.shape[-1] // (3 * heads)
            d_att[...] = dot(g_buf[k], w2[...], 1, 1).astype(BF)

            def one_seq(s, carry):
                r = pl.ds(pl.multiple_of(s * seq, seq), seq)
                for h in range(heads):
                    q = qkv[r, h * dim:(h + 1) * dim]
                    key = qkv[r, (heads + h) * dim:(heads + h + 1) * dim]
                    v = qkv[r, (2 * heads + h) * dim:(2 * heads + h + 1) * dim]
                    prob = aux[r, h * seq:(h + 1) * seq]
                    d_out = d_att[r, h * dim:(h + 1) * dim]
                    d_prob = dot(d_out, v, 1, 1).astype(BF).astype(F32)
                    row_dot = jnp.sum(d_prob * prob, axis=-1, keepdims=True)
                    d_score = (prob * (d_prob - row_dot) * scale).astype(BF)
                    dhid[slot, r, h * dim:(h + 1) * dim] = dot(d_score, key, 1, 0).astype(BF)
                    dhid[slot, r, (heads + h) * dim:(heads + h + 1) * dim] = dot(d_score, q, 0, 0).astype(BF)
                    dhid[slot, r, (2 * heads + h) * dim:(2 * heads + h + 1) * dim] = dot(
                        prob.astype(BF), d_out, 0, 0).astype(BF)
                return carry
            lax.fori_loop(0, GROUP, one_seq, 0, unroll=4)
        slot_free[k].append(save(k, 1, dhid.at[slot], dhid_out.at[pl.ds(k * rows, rows)]))
        send_partial(k, dhid.at[slot], w1, 1, s16, k16, 'n', 5)

    bufs = {'f': (k32, r32, x32, y32, 0), 'n': (k16, r16, x16, y16, 5)}

    def core_done(name, k):
        kb, rb, xb, yb, i = bufs[name]
        flight[name, k][0].wait_recv()
        if last:
            flight[name, k][0].wait_send()
            done.add(id(flight[name, k][0]))
        dt = kb.dtype
        for bx in (1, 0):
            for by in (1, 0):
                kb[k, bx, by] = (kb[k, bx, by].astype(F32) + rb[k, bx, by].astype(F32)).astype(dt)
        flight[name, k] = [remote(k, i + 1, kb.at[k, 1, :, :, cols_a], xb.at[k, :, :, cols_a], xax),
                           remote(k, i + 2, kb.at[k, :, 1, :, cols_b], xb.at[k, :, :, cols_b], yax)]

    def second_done(name, k):
        kb, rb, xb, yb, i = bufs[name]
        dt = kb.dtype
        copy_a, copy_b = flight[name, k]
        copy_a.wait_recv()
        for j in (1, 0):
            kb[k, 0, j, :, :CUT] = (kb[k, 0, j, :, :CUT].astype(F32) + xb[k, j, :, :CUT].astype(F32)).astype(dt)
        third_a = remote(k, i + 3, kb.at[k, 0, 1, :, cols_a], yb.at[k, :, cols_a], yax)
        copy_b.wait_recv()
        for j in (1, 0):
            kb[k, j, 0, :, CUT:] = (kb[k, j, 0, :, CUT:].astype(F32) + xb[k, j, :, CUT:].astype(F32)).astype(dt)
        third_b = remote(k, i + 4, kb.at[k, 1, 0, :, cols_b], yb.at[k, :, cols_b], xax)
        flight[name, k] = [third_a, third_b]

    def gather_start(name, k, quad, i):
        flight[name, k] = [
            remote(k, i, quad.at[k, 0, 0, :, cols_a], quad.at[k, 0, 1, :, cols_a], yax),
            remote(k, i + 1, quad.at[k, 0, 0, :, cols_b], quad.at[k, 1, 0, :, cols_b], xax)]

    def third_done(name, k):
        kb, rb, xb, yb, i = bufs[name]
        for copy in flight[name, k]:
            copy.wait_recv()
        summed = kb[k, 0, 0].astype(F32) + yb[k].astype(F32)
        if name == 'f':
            loads['own', 1, k].wait()
            value = own[1, k] - summed
            own[1, k] = value
            save(k, 2, own.at[1, k], res_out.at[k])
            quad_n[k, 0, 0] = value if last else rms_norm(value).astype(BF)
            gather_start('gn', k, quad_n, 10)
        else:
            loads['own', 0, k].wait()
            loads['own', 2, k].wait()
            x_in = own[0, k]
            inv = lax.rsqrt(jnp.mean(x_in * x_in, axis=-1, keepdims=True) + EPS)
            proj = jnp.mean(x_in * summed, axis=-1, keepdims=True)
            value = own[2, k] + (inv * summed - x_in * (inv * inv * inv * proj))
            own[2, k] = value
            save(k, 3, own.at[2, k], cot_out.at[k])
            quad_g[k, 0, 0] = value.astype(quad_g.dtype)
            gather_start('gg', k, quad_g, 15)

    def gather_second(name, k):
        quad, i = (quad_n, 10) if name == 'gn' else (quad_g, 15)
        copy_a, copy_b = flight[name, k]
        copy_a.wait_recv()
        second_a = remote(k, i + 2, quad.at[k, 0, :, :, cols_a], quad.at[k, 1, :, :, cols_a], xax)
        copy_b.wait_recv()
        second_b = remote(k, i + 3, quad.at[k, :, 0, :, cols_b], quad.at[k, :, 1, :, cols_b], yax)
        flight[name, k] = [second_a, second_b]

    arrivals = []

    def gather_core(name, k):
        quad, i, out = (quad_n, 10, next_n) if name == 'gn' else (quad_g, 15, next_g)
        for copy in flight[name, k]:
            copy.wait_recv()
        arrivals.append(remote(k, i + 4, quad.at[k], out.at[k, 1], core))
        save(k, 4 if name == 'gn' else 5, quad.at[k], out.at[k, 0])

    def compute(k):
        forward(k)
        backward(k)
        core_done('f', k)
        core_done('n', k)

    def stage(fn, k, a='f', b='n'):
        fn(a, k)
        fn(b, k)

    lags = [compute, lambda k: stage(second_done, k), lambda k: stage(third_done, k),
            lambda k: stage(gather_second, k, 'gn', 'gg'), lambda k: stage(gather_core, k, 'gn', 'gg')]
    for step in range(chunks + len(lags) - 1):
        for j, fn in enumerate(lags):
            k = step - j
            if 0 <= k < chunks:
                fn(k)

    for copy in arrivals:
        copy.wait_recv()
    for copy in sent:
        if id(copy) not in done:
            copy.wait_send()
    for copy in saved:
        if id(copy) not in done:
            copy.wait()


def run_half(kind, last, ident, n, g, w1, w2, base, res, cot, heads, scale):
    chunks, seq, width = base.shape
    rows = GROUP * seq
    hid = w2.shape[0]
    dhid = w1.shape[1]
    wide = F32 if last else BF
    total = chunks * rows
    gathered = jax.ShapeDtypeStruct((chunks, 2, 2, 2, seq, width), wide)
    own = jax.ShapeDtypeStruct((chunks, seq, width), F32)
    quad = (chunks, 2, 2, seq, width)
    small = (8, 128)
    mlp = kind == 'mlp'
    scratch = [pltpu.VMEM((chunks, rows, width), BF), pltpu.VMEM((chunks, rows, width), BF),
               pltpu.VMEM(w1.shape, BF), pltpu.VMEM(w2.shape, BF),
               pltpu.VMEM((3, chunks, seq, width), F32),
               pltpu.VMEM((2, rows, hid), BF), pltpu.VMEM((2, rows, dhid), BF),
               pltpu.VMEM((rows, hid if mlp else heads * seq), F32)]
    for dt in (F32, BF):
        scratch += [pltpu.VMEM(quad, dt)] * 3
        scratch += [pltpu.VMEM((chunks, 2, seq, width), dt), pltpu.VMEM((chunks, seq, width), dt)]
    scratch += [pltpu.VMEM(small if last else quad, BF)] * 2
    scratch += [pltpu.VMEM(small if mlp else (rows, dhid), BF), pltpu.VMEM(small if mlp else (rows, hid), BF)]
    scratch += [pltpu.SemaphoreType.DMA((2 + 5 * chunks,)), pltpu.SemaphoreType.DMA((chunks, 6)),
                pltpu.SemaphoreType.DMA((chunks, 20)), pltpu.SemaphoreType.DMA((chunks, 20))]
    any_spec = pl.BlockSpec(memory_space=pl.ANY)
    flops = 6 * total * width * (hid + dhid)
    return pl.pallas_call(
        functools.partial(half_block, kind, last, chunks, seq, heads, scale),
        out_shape=[gathered, gathered, own, own,
                   jax.ShapeDtypeStruct((total, hid), BF), jax.ShapeDtypeStruct((total, dhid), BF)],
        in_specs=[any_spec] * 7,
        out_specs=[any_spec] * 6,
        scratch_shapes=scratch,
        compiler_params=pltpu.CompilerParams(collective_id=ident, has_side_effects=True, vmem_limit_bytes=VMEM_LIMIT),
        cost_estimate=pl.CostEstimate(flops=flops, bytes_accessed=total * width * 12, transcendentals=total * hid),
        name=kind + ('_last' if last else ''),
    )(n, g, w1, w2, base, res, cot)


def order_blocks(blocks, me_bits):
    return jnp.concatenate([lax.dynamic_slice_in_dim(blocks, p ^ me_bits, 1, axis=1) for p in range(GROUP)], axis=1)


def solution(mesh):
    act_spec = P('dp')
    in_specs = (act_spec, act_spec, act_spec, act_spec,
                P(None, None, None, 'tp', None), P(None, 'tp', None, None),
                P(None, None, 'tp'), P(None, 'tp', None))
    out_specs = (act_spec, act_spec, act_spec, act_spec,
                 P('dp', None, None, 'tp', None), P('dp', 'tp', None, None),
                 P('dp', None, 'tp'), P('dp', 'tp', None))

    def device_body(y_one, y_two, dy_one, dy_two, w_qkv, w_out, w_up, w_down):
        n_micro, n_batch, seq, width = y_one.shape
        layers, heads, head_dim = w_qkv.shape[0], w_qkv.shape[3], w_qkv.shape[4]
        scale = head_dim ** -0.5
        pad = -head_dim % 128
        pdim = head_dim + pad
        chunks = n_micro * n_batch // GROUP
        total = chunks * GROUP * seq
        index = lax.axis_index('tp')
        me_bits = (index & 1) * 4 + (index & 2) + (index >> 2)

        full = [a.reshape(chunks, GROUP, seq, width) for a in (y_one, y_two, dy_one, dy_two)]
        one, two, g_one, g_two = [lax.dynamic_slice_in_dim(a, me_bits, 1, axis=1)[:, 0] for a in full]
        normed = order_blocks(rms_norm(full[0]).astype(BF), me_bits).reshape(total, width)
        grads = order_blocks(full[3].astype(BF), me_bits).reshape(total, width)

        w_qkv_p = jnp.pad(w_qkv, ((0, 0),) * 4 + ((0, pad),)).reshape(layers, width, 3 * heads * pdim)
        w_out_p = jnp.pad(w_out, ((0, 0), (0, 0), (0, pad), (0, 0))).reshape(layers, heads * pdim, width)

        d_qkv, d_out, d_up, d_down = [], [], [], []
        for layer in reversed(range(layers)):
            last = layer == 0
            nn, ng, two, g_one, act, d_pre = run_half(
                'mlp', last, 2 * last, normed, grads, w_up[layer], w_down[layer], one, two, g_one, heads, scale)
            d_down.append(dot(act, grads, 0, 0))
            d_up.append(dot(normed, d_pre, 0, 0))
            if last:
                nn, ng = (v.reshape(chunks, GROUP, seq, width) for v in (nn, ng))
                out_two, out_g_one = order_blocks(nn, me_bits), order_blocks(ng, me_bits)
                nn, ng = rms_norm(nn).astype(BF), ng.astype(BF)
            normed, grads = nn.reshape(total, width), ng.reshape(total, width)
            nn, ng, one, g_two, att, d_proj = run_half(
                'attn', last, 1 + 2 * last, normed, grads, w_qkv_p[layer], w_out_p[layer], two, one, g_two, heads, scale)
            d_out.append(dot(att, grads, 0, 0).reshape(heads, pdim, width)[:, :head_dim])
            d_qkv.append(dot(normed, d_proj, 0, 0).reshape(width, 3, heads, pdim)[..., :head_dim])
            if last:
                nn, ng = (v.reshape(chunks, GROUP, seq, width) for v in (nn, ng))
                out_one, out_g_two = order_blocks(nn, me_bits), order_blocks(ng, me_bits)
            normed, grads = nn.reshape(total, width), ng.reshape(total, width)

        acts = [v.reshape(y_one.shape) for v in (out_one, out_two, out_g_one, out_g_two)]
        return (*acts, jnp.stack(d_qkv[::-1]), jnp.stack(d_out[::-1]), jnp.stack(d_up[::-1]), jnp.stack(d_down[::-1]))

    return jax.shard_map(device_body, mesh=mesh, in_specs=in_specs, out_specs=out_specs, check_vma=False)
```

```python
import functools

import jax
import jax.numpy as jnp
from jax import lax
from jax.experimental import pallas as pl
from jax.experimental.pallas import tpu as pltpu
from jax.sharding import PartitionSpec as P

EPS = 1e-6
BF = jnp.bfloat16
F32 = jnp.float32
GROUP = 8
CUT = 896
GELU_K = 0.7978845608028654
MESH = pl.DeviceIdType.MESH
VMEM_LIMIT = 67043328


def rms_norm(x_in):
    return x_in * lax.rsqrt(jnp.mean(x_in * x_in, axis=-1, keepdims=True) + EPS)


def dot(a, b, ca, cb):
    return lax.dot_general(a, b, (((ca,), (cb,)), ((), ())), preferred_element_type=F32)


def tiles(total, size, body):
    def step(i, carry):
        body(pl.multiple_of(i * size, size), size)
        return carry
    lax.fori_loop(0, total // size, step, 0)
    if total % size:
        body(total // size * size, total % size)


def backward_pass(layers, chunks, seq, heads, dim, scale, *refs):
    (y1, y2, dy1, dy2, wa_hbm, wu_hbm, wd_hbm,
     x1, x2, dx1, dx2, dwa, dwu, dwd, next_n, next_g,
     n_buf, g_buf, w1, w2, own, hid, dhid, aux, s32, k32, r32, x32, y32, s16, k16, r16, x16, y16,
     quad_n, quad_g, in_sem, first_sem, own_sem, w_sem, wg_sem, out_sem, send_sem, recv_sem, fsend_sem, frecv_sem) = refs
    width = n_buf.shape[-1]
    rows = GROUP * seq
    half = rows // 2
    att_w = heads * dim
    me = lax.axis_index('tp')
    my_core, my_x, my_y = lax.rem(me, 2), lax.rem(lax.div(me, 2), 2), lax.rem(lax.div(me, 4), 2)
    core, xax, yax = {'tp': me + 1 - 2 * my_core}, {'tp': me + 2 - 4 * my_x}, {'tp': me + 4 - 8 * my_y}

    barrier = pltpu.get_barrier_semaphore()
    for dev in (core, xax, yax):
        pl.semaphore_signal(barrier, inc=1, device_id=dev, device_id_type=MESH)

    def local(src, dst, sem):
        copy = pltpu.make_async_copy(src, dst, sem)
        copy.start()
        return copy

    loads = {}

    def load_weights(h):
        layer = layers - 1 - h // 2
        if h % 2 == 0:
            loads['w1'] = local(wu_hbm.at[layer], w1, w_sem.at[0])
            loads['w2'] = local(wd_hbm.at[layer], w2, w_sem.at[1])
        else:
            loads['w2'] = local(wa_hbm.at[layer], w2, w_sem.at[1])

    def place(k, c, bx, by):
        return k * GROUP + 4 * (my_core + c - 2 * c * my_core) + 2 * (my_x + bx - 2 * bx * my_x) + (
            my_y + by - 2 * by * my_y)

    firsts = [(k, src) for k in range(chunks) for src in (0, 1)]

    def fetch_first(i):
        k, src = firsts[i]
        slot = 1 + src
        loads['first', i] = [
            local((dy2 if src else y1).at[place(k, c, b // 2, b % 2)], (k32 if c else s32).at[slot, b // 2, b % 2],
                  first_sem.at[src, 4 * c + b]) for c in range(2) for b in range(4)]

    def round_first(i):
        k, src = firsts[i]
        slot = 1 + src
        for copy in loads.pop(('first', i)):
            copy.wait()
        for c in range(2):
            def one(b, carry):
                value = (k32 if c else s32)[slot, lax.div(b, 2), lax.rem(b, 2)]
                if src == 0:
                    n_buf[k, c, lax.div(b, 2), lax.rem(b, 2)] = rms_norm(value).astype(BF)
                else:
                    g_buf[k, c, lax.div(b, 2), lax.rem(b, 2)] = value.astype(BF)
                return carry
            lax.fori_loop(0, 4, one, 0)
        if i + 2 < len(firsts):
            fetch_first(i + 2)

    fetch_first(0)
    load_weights(0)
    fetch_first(1)
    mine = place(0, 0, 0, 0)
    for k in range(chunks):
        for j, src in enumerate((y1, y2, dy1, dy2)):
            loads['own', j, k] = local(src.at[k * GROUP + mine], own.at[j, k], own_sem.at[k, j])
    pl.semaphore_wait(barrier, 3)
    round_first(0)
    round_first(1)

    sends = [[] for _ in range(chunks)]
    flight, arrivals, staged = {}, {}, {}

    def remote(k, i, src, dst, dev):
        copy = pltpu.make_async_remote_copy(src_ref=src, dst_ref=dst, send_sem=send_sem.at[k, i],
                                            recv_sem=recv_sem.at[k, i], device_id=dev, device_id_type=MESH)
        copy.start()
        sends[k].append(copy)
        return copy

    def done_once(key):
        for copy in loads.pop(key, ()):
            copy.wait()

    cols_a, cols_b = pl.ds(0, CUT), pl.ds(CUT, width - CUT)
    bufs = {'f': (s32, k32, r32, x32, y32, 0), 'n': (s16, k16, r16, x16, y16, 5)}

    def send_partial(k, lhs, depth, weight, name):
        s_ref, k_ref, r_ref, _, _, i = bufs[name]

        def make(out, part):
            def tile(off, size):
                a = lhs[part * half:(part + 1) * half, :depth]
                b, cb = weight(off, size)
                out[k, :, :, :, pl.ds(off, size)] = dot(a, b, 1, cb).astype(out.dtype).reshape(2, 2, seq, size)
            tiles(width, 256, tile)
        make(s_ref, 1)
        flight[name, k] = [remote(k, i, s_ref.at[k], r_ref.at[k], core)]
        make(k_ref, 0)

    def chunk_of(buf, k):
        return buf[k].reshape(rows, width)

    def compute(t):
        h, k = divmod(t, chunks)
        mlp = h % 2 == 0
        if h > 0:
            for name, quad, nxt, buf, j in (('gn', quad_n, next_n, n_buf, 0), ('gg', quad_g, next_g, g_buf, 2)):
                first = local(quad.at[k], buf.at[k, 0], in_sem.at[k, j])
                arrivals.pop((name, k)).wait_recv()
                loads[name[1], k] = [first, local(nxt.at[k], buf.at[k, 1], in_sem.at[k, j + 1])]
            for copy in sends[k]:
                copy.wait_send()
            sends[k].clear()
        if k == 0:
            loads['w1' if mlp else 'w2'].wait()
        done_once(('n', k))
        if mlp:
            def up_tile(off, size):
                u = dot(chunk_of(n_buf, k), w1[:, pl.ds(off, size)], 1, 0)
                t_u = jnp.tanh(GELU_K * (u + 0.044715 * u * u * u))
                hid[k, :, pl.ds(off, size)] = (0.5 * u * (1.0 + t_u)).astype(BF)
                aux[:, pl.ds(off, size)] = 0.5 * (1.0 + t_u) + 0.5 * u * (1.0 - t_u * t_u) * (
                    GELU_K * (1.0 + 3 * 0.044715 * u * u))
            tiles(hid.shape[-1], 256, up_tile)
        else:
            def qkv_tile(off, size):
                hid[k, :, pl.ds(att_w + off, size)] = dot(chunk_of(n_buf, k), w2[pl.ds(off, size), :], 1, 1).astype(BF)
            tiles(3 * att_w, 256, qkv_tile)

            def fwd_seq(s, carry):
                r = pl.ds(pl.multiple_of(s * seq, seq), seq)
                for i in range(heads):
                    q, key, v = (hid[k, r, (j * heads + heads + i) * dim:(j * heads + heads + i + 1) * dim] for j in range(3))
                    scores = dot(q, key, 1, 1) * scale
                    expd = jnp.exp(scores - jnp.max(scores, axis=-1, keepdims=True))
                    prob = expd / jnp.sum(expd, axis=-1, keepdims=True)
                    aux[r, i * seq:(i + 1) * seq] = prob
                    hid[k, r, i * dim:(i + 1) * dim] = dot(prob.astype(BF), v, 1, 0).astype(BF)
                return carry
            lax.fori_loop(0, GROUP, fwd_seq, 0, unroll=4)
        if k == 0 and mlp:
            loads['w2'].wait()
        row0, depth = (0, hid.shape[-1]) if mlp else (3 * att_w, att_w)
        send_partial(k, hid.at[k], depth, lambda off, size: (w2[row0:row0 + depth, pl.ds(off, size)], 0), 'f')
        done_once(('g', k))
        if mlp:
            def down_tile(off, size):
                d_act = dot(chunk_of(g_buf, k), w2[pl.ds(off, size), :], 1, 1)
                dhid[k, :, pl.ds(off, size)] = (d_act * aux[:, pl.ds(off, size)]).astype(BF)
            tiles(dhid.shape[-1], 256, down_tile)
        else:
            dhid[k, :, 3 * att_w:4 * att_w] = dot(chunk_of(g_buf, k), w2[3 * att_w:, :], 1, 1).astype(BF)

            def bwd_seq(s, carry):
                r = pl.ds(pl.multiple_of(s * seq, seq), seq)
                for i in range(heads):
                    q, key, v = (hid[k, r, (j * heads + heads + i) * dim:(j * heads + heads + i + 1) * dim] for j in range(3))
                    prob = aux[r, i * seq:(i + 1) * seq]
                    d_out = dhid[k, r, 3 * att_w + i * dim:3 * att_w + (i + 1) * dim]
                    d_prob = dot(d_out, v, 1, 1).astype(BF).astype(F32)
                    row_dot = jnp.sum(d_prob * prob, axis=-1, keepdims=True)
                    d_score = (prob * (d_prob - row_dot) * scale).astype(BF)
                    parts = (dot(d_score, key, 1, 0), dot(d_score, q, 0, 0), dot(prob.astype(BF), d_out, 0, 0))
                    for j, part in enumerate(parts):
                        dhid[k, r, (j * heads + i) * dim:(j * heads + i + 1) * dim] = part.astype(BF)
                return carry
            lax.fori_loop(0, GROUP, bwd_seq, 0, unroll=4)
        if mlp:
            send_partial(k, dhid.at[k], dhid.shape[-1], lambda off, size: (w1[pl.ds(off, size), :], 1), 'n')
        else:
            send_partial(k, dhid.at[k], 3 * att_w, lambda off, size: (w2[:3 * att_w, pl.ds(off, size)], 0), 'n')
        if k == chunks - 1 and h + 1 < 2 * layers:
            load_weights(h + 1)
        core_done('f', t)
        core_done('n', t)

    def is_last(t):
        return t // chunks >= 2 * layers - 2

    def core_done(name, t):
        k = t % chunks
        _, kb, rb, xb, yb, i = bufs[name]
        flight[name, k][0].wait_recv()
        if is_last(t):
            flight[name, k][0].wait_send()
            sends[k] = [copy for copy in sends[k] if copy is not flight[name, k][0]]
        dt = kb.dtype
        for bx in (1, 0):
            for by in (1, 0):
                kb[k, bx, by] = (kb[k, bx, by].astype(F32) + rb[k, bx, by].astype(F32)).astype(dt)
        flight[name, k] = [remote(k, i + 1, kb.at[k, 1, :, :, cols_a], xb.at[k, :, :, cols_a], xax),
                           remote(k, i + 2, kb.at[k, :, 1, :, cols_b], xb.at[k, :, :, cols_b], yax)]

    def second_done(name, t):
        k = t % chunks
        _, kb, rb, xb, yb, i = bufs[name]
        dt = kb.dtype
        copy_a, copy_b = flight[name, k]
        copy_a.wait_recv()
        for j in (1, 0):
            kb[k, 0, j, :, :CUT] = (kb[k, 0, j, :, :CUT].astype(F32) + xb[k, j, :, :CUT].astype(F32)).astype(dt)
        third_a = remote(k, i + 3, kb.at[k, 0, 1, :, cols_a], yb.at[k, :, cols_a], yax)
        copy_b.wait_recv()
        for j in (1, 0):
            kb[k, j, 0, :, CUT:] = (kb[k, j, 0, :, CUT:].astype(F32) + xb[k, j, :, CUT:].astype(F32)).astype(dt)
        third_b = remote(k, i + 4, kb.at[k, 1, 0, :, cols_b], yb.at[k, :, cols_b], xax)
        flight[name, k] = [third_a, third_b]

    def quads(name, t):
        if is_last(t):
            return (s32, 10) if name == 'gn' else (r32, 15)
        return (quad_n, 10) if name == 'gn' else (quad_g, 15)

    def gather_start(name, t):
        k = t % chunks
        quad, i = quads(name, t)
        flight[name, k] = [
            remote(k, i, quad.at[k, 0, 0, :, cols_a], quad.at[k, 0, 1, :, cols_a], yax),
            remote(k, i + 1, quad.at[k, 0, 0, :, cols_b], quad.at[k, 1, 0, :, cols_b], xax)]

    def third_done(name, t):
        h, k = divmod(t, chunks)
        base, res, cot = (0, 1, 2) if h % 2 == 0 else (1, 0, 3)
        _, kb, rb, xb, yb, i = bufs[name]
        for copy in flight[name, k]:
            copy.wait_recv()
        summed = kb[k, 0, 0].astype(F32) + yb[k].astype(F32)
        for j in range(4):
            if ('own', j, k) in loads:
                loads.pop(('own', j, k)).wait()
        if name == 'f':
            value = own[res, k] - summed
            own[res, k] = value
            quad = quads('gn', t)[0]
            quad[k, 0, 0] = value if is_last(t) else rms_norm(value).astype(BF)
            gather_start('gn', t)
        else:
            x_in = own[base, k]
            inv = lax.rsqrt(jnp.mean(x_in * x_in, axis=-1, keepdims=True) + EPS)
            proj = jnp.mean(x_in * summed, axis=-1, keepdims=True)
            value = own[cot, k] + (inv * summed - x_in * (inv * inv * inv * proj))
            own[cot, k] = value
            quad = quads('gg', t)[0]
            quad[k, 0, 0] = value.astype(quad.dtype)
            gather_start('gg', t)

    def gather_second(name, t):
        k = t % chunks
        quad, i = quads(name, t)
        copy_a, copy_b = flight[name, k]
        copy_a.wait_recv()
        second_a = remote(k, i + 2, quad.at[k, 0, :, :, cols_a], quad.at[k, 1, :, :, cols_a], xax)
        copy_b.wait_recv()
        second_b = remote(k, i + 3, quad.at[k, :, 0, :, cols_b], quad.at[k, :, 1, :, cols_b], yax)
        flight[name, k] = [second_a, second_b]

    finals = []

    def gather_core(t):
        h, k = divmod(t, chunks)
        more = h + 1 < 2 * layers
        for name in ('gn', 'gg'):
            for copy in flight[name, k]:
                copy.wait_recv()
        if is_last(t):
            leaving = []
            outs = (x2, dx1) if h % 2 == 0 else (x1, dx2)
            for j, (name, out) in enumerate(zip(('gn', 'gg'), outs)):
                quad = quads(name, t)[0]
                for b in range(4):
                    bx, by = divmod(b, 2)
                    there = place(k, 0, bx, by)
                    far = pltpu.make_async_remote_copy(
                        src_ref=quad.at[k, bx, by], dst_ref=out.at[there], send_sem=fsend_sem.at[k, 4 * j + b],
                        recv_sem=frecv_sem.at[k, 4 * j + b], device_id=core, device_id_type=MESH)
                    far.start()
                    leaving.append((far, local(quad.at[k, bx, by], out.at[there], out_sem.at[k, 4 * j + b])))
            if more:
                for b in range(4):
                    bx, by = divmod(b, 2)
                    quad_n[k, bx, by] = rms_norm(s32[k, bx, by]).astype(BF)
                    quad_g[k, bx, by] = r32[k, bx, by].astype(BF)
                for far, near in leaving:
                    far.wait()
                    near.wait()
                for copy in sends[k]:
                    copy.wait_send()
                sends[k].clear()
            else:
                finals.extend(leaving)
        if more:
            arrivals['gn', k] = remote(k, 14, quad_n.at[k], next_n.at[k], core)
            arrivals['gg', k] = remote(k, 19, quad_g.at[k], next_g.at[k], core)

    def stage(slot, shape, dst):
        return pltpu.make_async_copy(aux.at[pl.ds(slot * 256, shape[0]), pl.ds(0, shape[1])], dst, wg_sem.at[slot])

    def weight_grads(h):
        layer = layers - 1 - h // 2
        mlp = h % 2 == 0
        total = chunks * rows

        def put(slot, value, dst, wait):
            copy = stage(slot, value.shape, dst)
            if wait is None:
                copy.wait()
            else:
                @pl.when(wait)
                def _():
                    copy.wait()
            aux[slot * 256:slot * 256 + value.shape[0], :value.shape[1]] = value
            copy.start()

        def wide(lhs, rhs, out, row0, lo, hi):
            def body(i, carry):
                off = pl.multiple_of(i * 256, 256)
                a = lhs[:, :, pl.ds(off, 256)].reshape(total, 256)
                for slot, (c0, cw) in enumerate(((0, CUT), (CUT, width - CUT))):
                    b = rhs[:, :, :, :, :, c0:c0 + cw].reshape(total, cw)
                    put(slot, dot(a, b, 0, 0), out.at[layer, pl.ds(row0 + off, 256), pl.ds(c0, cw)], i > lo)
                return carry
            lax.fori_loop(lo, hi, body, 0)
            for slot, (c0, cw) in enumerate(((0, CUT), (CUT, width - CUT))):
                stage(slot, (256, cw), out.at[layer, pl.ds(row0, 256), pl.ds(c0, cw)]).wait()

        def tall(lo, hi, size=256):
            cw = dhid.shape[-1] // 2

            def body(i, carry):
                off = i * 256 if size != 256 else pl.multiple_of(i * 256, 256)
                a = n_buf[:, :, :, :, :, pl.ds(off, size)].reshape(total, size)
                for slot in range(2):
                    b = dhid[:, :, slot * cw:(slot + 1) * cw].reshape(total, cw)
                    put(slot, dot(a, b, 0, 0), dwu.at[layer, pl.ds(off, size), pl.ds(slot * cw, cw)], i > lo)
                return carry
            if size == 256:
                lax.fori_loop(lo, hi, body, 0)
            else:
                body(lo, 0)
            for slot in range(2):
                stage(slot, (size, cw), dwu.at[layer, pl.ds(0, size), pl.ds(slot * cw, cw)]).wait()

        if not mlp:
            cut = 3 * att_w // 512
            return [lambda: wide(dhid, n_buf, dwa, 0, 0, cut), lambda: wide(dhid, n_buf, dwa, 0, cut, 3 * att_w // 256),
                    lambda: wide(hid, g_buf, dwa, 3 * att_w, 0, att_w // 256)]
        deep, high = hid.shape[-1] // 256, width // 256
        pieces = [lambda: wide(hid, g_buf, dwd, 0, 0, deep // 2), lambda: wide(hid, g_buf, dwd, 0, deep // 2, deep),
                  lambda: tall(0, high // 2), lambda: tall(high // 2, high)]
        if width % 256:
            pieces.append(lambda: tall(high, high, width % 256))
        return pieces

    tasks = 2 * layers * chunks
    for t in range(tasks + 2):
        pieces = []
        if t == 1:
            for i in range(2, len(firsts)):
                round_first(i)
        if t < tasks:
            compute(t)
            if t % chunks == chunks - 1:
                pieces = weight_grads(t // chunks)
        if 0 <= t - 1 < tasks:
            third_done('f', t - 1)
            third_done('n', t - 1)
        for piece in pieces[:2]:
            piece()
        if 0 <= t - 2 < tasks:
            gather_core(t - 2)
        for piece in pieces[2:3]:
            piece()
        if t < tasks:
            second_done('f', t)
            second_done('n', t)
        if 0 <= t - 1 < tasks:
            gather_second('gn', t - 1)
            gather_second('gg', t - 1)
        for piece in pieces[3:]:
            piece()
    for far, near in finals:
        far.wait()
        near.wait()
    for k in range(chunks):
        for copy in sends[k]:
            copy.wait_send()


def run_stack(acts, w_att, w_up, w_down, heads, scale):
    layers, width, hid = w_up.shape
    att_w = w_att.shape[1] // 4
    seq = acts[0].shape[1]
    chunks = acts[0].shape[0] // GROUP
    rows = GROUP * seq
    quad = (chunks, 2, 2, seq, width)
    oct_ = (chunks, 2, 2, 2, seq, width)
    scratch = [pltpu.VMEM(oct_, BF), pltpu.VMEM(oct_, BF), pltpu.VMEM((width, hid), BF), pltpu.VMEM((hid, width), BF),
               pltpu.VMEM((4, chunks, seq, width), F32),
               pltpu.VMEM((chunks, rows, hid), BF), pltpu.VMEM((chunks, rows, hid), BF),
               pltpu.VMEM((rows, hid), F32)]
    for dt in (F32, BF):
        scratch += [pltpu.VMEM(quad, dt)] * 3
        scratch += [pltpu.VMEM((chunks, 2, seq, width), dt), pltpu.VMEM((chunks, seq, width), dt)]
    scratch += [pltpu.VMEM(quad, BF)] * 2
    dma = pltpu.SemaphoreType.DMA
    scratch += [dma((chunks, 4)), dma((2, 8)), dma((chunks, 4)), dma((2,)), dma((2,)), dma((chunks, 8)),
                dma((chunks, 20)), dma((chunks, 20)), dma((chunks, 8)), dma((chunks, 8))]
    any_spec = pl.BlockSpec(memory_space=pl.ANY)
    outs = [jax.ShapeDtypeStruct(a.shape, F32) for a in acts]
    outs += [jax.ShapeDtypeStruct(w.shape, F32) for w in (w_att, w_up, w_down)]
    outs += [jax.ShapeDtypeStruct(quad, BF)] * 2
    return pl.pallas_call(
        functools.partial(backward_pass, layers, chunks, seq, heads, att_w // heads, scale),
        out_shape=outs,
        in_specs=[any_spec] * 7,
        out_specs=[any_spec] * 9,
        scratch_shapes=scratch,
        compiler_params=pltpu.CompilerParams(collective_id=0, has_side_effects=True, vmem_limit_bytes=VMEM_LIMIT),
        name='backward_pass',
    )(*acts, w_att, w_up, w_down)


def copy_out(heads_att, head_dim, *refs):
    ins, outs = refs[:7], refs[7:]
    for src, dst in zip(ins[:6], outs[:6]):
        dst[...] = src[...]
    place = lax.rem(pl.program_id(0), heads_att)
    dq, do = outs[6:]

    @pl.when(place < 3 * heads_att // 4)
    def _():
        dq[...] = ins[6][:, :head_dim]

    @pl.when(place >= 3 * heads_att // 4)
    def _():
        do[...] = ins[6][:, :head_dim]


def write_results(acts, dwu, dwd, dwa, heads, head_dim):
    steps, seq, width = acts[0].shape
    layers = dwu.shape[0]
    per = steps // layers
    each = 4 * heads
    dwa = dwa.reshape(layers * each, -1, width)

    def split(a):
        return a.reshape(steps, -1, a.shape[-1])
    arrays = [*acts, split(dwu), split(dwd), dwa]

    def whole(a):
        return pl.BlockSpec((1,) + a.shape[1:], lambda i: (i, 0, 0))
    q_spec = pl.BlockSpec((1, head_dim, width), lambda i: (i // each * 3 * heads + jnp.minimum(i % each, 3 * heads - 1), 0, 0))
    o_spec = pl.BlockSpec((1, head_dim, width), lambda i: (i // each * heads + jnp.maximum(i % each - 3 * heads, 0), 0, 0))
    outs = pl.pallas_call(
        functools.partial(copy_out, each, head_dim),
        grid=(steps,),
        in_specs=[whole(a) for a in arrays],
        out_specs=[whole(a) for a in arrays[:6]] + [q_spec, o_spec],
        out_shape=[jax.ShapeDtypeStruct(a.shape, F32) for a in arrays[:6]] + [
            jax.ShapeDtypeStruct((layers * 3 * heads, head_dim, width), F32),
            jax.ShapeDtypeStruct((layers * heads, head_dim, width), F32)],
        compiler_params=pltpu.CompilerParams(vmem_limit_bytes=VMEM_LIMIT),
        name='write_results',
    )(*arrays)
    return (*outs[:4], outs[4].reshape(dwu.shape), outs[5].reshape(dwd.shape),
            outs[6].reshape(layers, 3, heads, head_dim, width), outs[7].reshape(layers, heads, head_dim, width))


def solution(mesh):
    act_spec = P('dp')
    in_specs = (act_spec, act_spec, act_spec, act_spec,
                P(None, None, None, 'tp', None), P(None, 'tp', None, None),
                P(None, None, 'tp'), P(None, 'tp', None))
    out_specs = (act_spec, act_spec, act_spec, act_spec,
                 P('dp', None, None, 'tp', None), P('dp', 'tp', None, None),
                 P('dp', None, 'tp'), P('dp', 'tp', None))

    def device_body(y_one, y_two, dy_one, dy_two, w_qkv, w_out, w_up, w_down):
        n_micro, n_batch, seq, width = y_one.shape
        layers, heads, head_dim = w_qkv.shape[0], w_qkv.shape[3], w_qkv.shape[4]
        pad = -head_dim % 128
        pdim = head_dim + pad
        chunks = n_micro * n_batch // GROUP
        acts = [a.reshape(chunks * GROUP, seq, width) for a in (y_one, y_two, dy_one, dy_two)]
        w_q = jnp.pad(w_qkv.transpose(0, 2, 3, 4, 1).reshape(layers, 3 * heads, head_dim, width), ((0, 0), (0, 0), (0, pad), (0, 0)))
        w_o = jnp.pad(w_out, ((0, 0), (0, 0), (0, pad), (0, 0)))
        w_att = jnp.concatenate([w_q, w_o], axis=1).reshape(layers, 4 * heads * pdim, width)
        x1, x2, dx1, dx2, dwa, dwu, dwd, _, _ = run_stack(acts, w_att, w_up, w_down, heads, head_dim ** -0.5)
        x1, x2, dx1, dx2, dwu, dwd, dwq, dwo = write_results((x1, x2, dx1, dx2), dwu, dwd, dwa, heads, head_dim)
        return (*(a.reshape(y_one.shape) for a in (x1, x2, dx1, dx2)), dwq.transpose(0, 4, 1, 2, 3), dwo, dwu, dwd)

    return jax.shard_map(device_body, mesh=mesh, in_specs=in_specs, out_specs=out_specs, check_vma=False)
```

```python
import functools

import jax
import jax.numpy as jnp
from jax import lax
from jax.experimental import pallas as pl
from jax.experimental.pallas import tpu as pltpu
from jax.sharding import PartitionSpec as P

EPS = 1e-6
BF = jnp.bfloat16
F32 = jnp.float32
GROUP = 8
CUT = 896
GELU_K = 0.7978845608028654
MESH = pl.DeviceIdType.MESH
VMEM_LIMIT = 67043328


def rms_norm(x_in):
    return x_in * lax.rsqrt(jnp.mean(x_in * x_in, axis=-1, keepdims=True) + EPS)


def dot(a, b, ca, cb):
    return lax.dot_general(a, b, (((ca,), (cb,)), ((), ())), preferred_element_type=F32)


def tiles(total, size, body):
    def step(i, carry):
        body(pl.multiple_of(i * size, size), size)
        return carry
    lax.fori_loop(0, total // size, step, 0)
    if total % size:
        body(total // size * size, total % size)


def backward_pass(layers, chunks, seq, heads, dim, scale, *refs):
    (y1, y2, dy1, dy2, wa_hbm, wu_hbm, wd_hbm,
     x1, x2, dx1, dx2, dwa, dwu, dwd, next_n, next_g,
     n_buf, g_buf, w1, w2, own, hid, dhid, aux, s32, k32, r32, x32, y32, s16, k16, r16, x16, y16,
     quad_n, quad_g, in_sem, first_sem, own_sem, w_sem, wg_sem, out_sem, send_sem, recv_sem, fsend_sem, frecv_sem) = refs
    width = n_buf.shape[-1]
    rows = GROUP * seq
    half = rows // 2
    att_w = heads * dim
    me = lax.axis_index('tp')
    my_core, my_x, my_y = lax.rem(me, 2), lax.rem(lax.div(me, 2), 2), lax.rem(lax.div(me, 4), 2)
    core, xax, yax = {'tp': me + 1 - 2 * my_core}, {'tp': me + 2 - 4 * my_x}, {'tp': me + 4 - 8 * my_y}

    barrier = pltpu.get_barrier_semaphore()
    for dev in (core, xax, yax):
        pl.semaphore_signal(barrier, inc=1, device_id=dev, device_id_type=MESH)

    def local(src, dst, sem):
        copy = pltpu.make_async_copy(src, dst, sem)
        copy.start()
        return copy

    loads = {}

    def load_weights(h):
        layer = layers - 1 - h // 2
        if h % 2 == 0:
            loads['w1'] = local(wu_hbm.at[layer], w1, w_sem.at[0])
            loads['w2'] = local(wd_hbm.at[layer], w2, w_sem.at[1])
        else:
            loads['w2'] = local(wa_hbm.at[layer], w2, w_sem.at[1])

    def place(k, c, bx, by):
        return k * GROUP + 4 * (my_core + c - 2 * c * my_core) + 2 * (my_x + bx - 2 * bx * my_x) + (
            my_y + by - 2 * by * my_y)

    firsts = [(k, src) for k in range(chunks) for src in (0, 1)]

    def fetch_first(i):
        k, src = firsts[i]
        slot = 1 + src
        loads['first', i] = [
            local((dy2 if src else y1).at[place(k, c, b // 2, b % 2)], (k32 if c else s32).at[slot, b // 2, b % 2],
                  first_sem.at[src, 4 * c + b]) for c in range(2) for b in range(4)]

    def round_first(i):
        k, src = firsts[i]
        slot = 1 + src
        for copy in loads.pop(('first', i)):
            copy.wait()
        for c in range(2):
            def one(b, carry):
                value = (k32 if c else s32)[slot, lax.div(b, 2), lax.rem(b, 2)]
                if src == 0:
                    n_buf[k, c, lax.div(b, 2), lax.rem(b, 2)] = rms_norm(value).astype(BF)
                else:
                    g_buf[k, c, lax.div(b, 2), lax.rem(b, 2)] = value.astype(BF)
                return carry
            lax.fori_loop(0, 4, one, 0)
        if i + 2 < len(firsts):
            fetch_first(i + 2)

    fetch_first(0)
    load_weights(0)
    fetch_first(1)
    mine = place(0, 0, 0, 0)
    for k in range(chunks):
        for j, src in enumerate((y1, y2, dy1, dy2)):
            loads['own', j, k] = local(src.at[k * GROUP + mine], own.at[j, k], own_sem.at[k, j])
    pl.semaphore_wait(barrier, 3)
    round_first(0)
    round_first(1)

    sends = [[] for _ in range(chunks)]
    flight, arrivals, staged = {}, {}, {}

    def remote(k, i, src, dst, dev):
        copy = pltpu.make_async_remote_copy(src_ref=src, dst_ref=dst, send_sem=send_sem.at[k, i],
                                            recv_sem=recv_sem.at[k, i], device_id=dev, device_id_type=MESH)
        copy.start()
        sends[k].append(copy)
        return copy

    def done_once(key):
        for copy in loads.pop(key, ()):
            copy.wait()

    cols_a, cols_b = pl.ds(0, CUT), pl.ds(CUT, width - CUT)
    bufs = {'f': (s32, k32, r32, x32, y32, 0), 'n': (s16, k16, r16, x16, y16, 5)}

    def send_partial(k, lhs, depth, weight, name):
        s_ref, k_ref, r_ref, _, _, i = bufs[name]

        def make(out, part):
            def tile(off, size):
                a = lhs[part * half:(part + 1) * half, :depth]
                b, cb = weight(off, size)
                out[k, :, :, :, pl.ds(off, size)] = dot(a, b, 1, cb).astype(out.dtype).reshape(2, 2, seq, size)
            tiles(width, 256, tile)
        make(s_ref, 1)
        flight[name, k] = [remote(k, i, s_ref.at[k], r_ref.at[k], core)]
        make(k_ref, 0)

    def chunk_of(buf, k):
        return buf[k].reshape(rows, width)

    def compute(t):
        h, k = divmod(t, chunks)
        mlp = h % 2 == 0
        if h > 0:
            for name, quad, nxt, buf, j in (('gn', quad_n, next_n, n_buf, 0), ('gg', quad_g, next_g, g_buf, 2)):
                first = local(quad.at[k], buf.at[k, 0], in_sem.at[k, j])
                arrivals.pop((name, k)).wait_recv()
                loads[name[1], k] = [first, local(nxt.at[k], buf.at[k, 1], in_sem.at[k, j + 1])]
            for copy in sends[k]:
                copy.wait_send()
            sends[k].clear()
        if k == 0:
            loads['w1' if mlp else 'w2'].wait()
        done_once(('n', k))
        if mlp:
            def up_tile(off, size):
                u = dot(chunk_of(n_buf, k), w1[:, pl.ds(off, size)], 1, 0)
                t_u = jnp.tanh(GELU_K * (u + 0.044715 * u * u * u))
                hid[k, :, pl.ds(off, size)] = (0.5 * u * (1.0 + t_u)).astype(BF)
                aux[:, pl.ds(off, size)] = 0.5 * (1.0 + t_u) + 0.5 * u * (1.0 - t_u * t_u) * (
                    GELU_K * (1.0 + 3 * 0.044715 * u * u))
            tiles(hid.shape[-1], 256, up_tile)
        else:
            def qkv_tile(off, size):
                hid[k, :, pl.ds(att_w + off, size)] = dot(chunk_of(n_buf, k), w2[pl.ds(off, size), :], 1, 1).astype(BF)
            tiles(3 * att_w, 256, qkv_tile)

            def fwd_seq(s, carry):
                r = pl.ds(pl.multiple_of(s * seq, seq), seq)
                for i in range(heads):
                    q, key, v = (hid[k, r, (j * heads + heads + i) * dim:(j * heads + heads + i + 1) * dim] for j in range(3))
                    scores = dot(q, key, 1, 1) * scale
                    expd = jnp.exp(scores - jnp.max(scores, axis=-1, keepdims=True))
                    prob = expd / jnp.sum(expd, axis=-1, keepdims=True)
                    aux[r, i * 128:i * 128 + seq] = prob
                    hid[k, r, i * dim:(i + 1) * dim] = dot(prob.astype(BF), v, 1, 0).astype(BF)
                return carry
            lax.fori_loop(0, GROUP, fwd_seq, 0, unroll=4)
        if k == 0 and mlp:
            loads['w2'].wait()
        row0, depth = (0, hid.shape[-1]) if mlp else (3 * att_w, att_w)
        send_partial(k, hid.at[k], depth, lambda off, size: (w2[row0:row0 + depth, pl.ds(off, size)], 0), 'f')
        done_once(('g', k))
        if mlp:
            def down_tile(off, size):
                d_act = dot(chunk_of(g_buf, k), w2[pl.ds(off, size), :], 1, 1)
                dhid[k, :, pl.ds(off, size)] = (d_act * aux[:, pl.ds(off, size)]).astype(BF)
            tiles(dhid.shape[-1], 256, down_tile)
        else:
            dhid[k, :, 3 * att_w:4 * att_w] = dot(chunk_of(g_buf, k), w2[3 * att_w:, :], 1, 1).astype(BF)

            def bwd_seq(s, carry):
                r = pl.ds(pl.multiple_of(s * seq, seq), seq)
                for i in range(heads):
                    q, key, v = (hid[k, r, (j * heads + heads + i) * dim:(j * heads + heads + i + 1) * dim] for j in range(3))
                    prob = aux[r, i * 128:i * 128 + seq]
                    d_out = dhid[k, r, 3 * att_w + i * dim:3 * att_w + (i + 1) * dim]
                    d_prob = dot(d_out, v, 1, 1).astype(BF).astype(F32)
                    row_dot = jnp.sum(d_prob * prob, axis=-1, keepdims=True)
                    d_score = (prob * (d_prob - row_dot) * scale).astype(BF)
                    parts = (dot(d_score, key, 1, 0), dot(d_score, q, 0, 0), dot(prob.astype(BF), d_out, 0, 0))
                    for j, part in enumerate(parts):
                        dhid[k, r, (j * heads + i) * dim:(j * heads + i + 1) * dim] = part.astype(BF)
                return carry
            lax.fori_loop(0, GROUP, bwd_seq, 0, unroll=4)

    def compute_rest(t):
        h, k = divmod(t, chunks)
        if h % 2 == 0:
            send_partial(k, dhid.at[k], dhid.shape[-1], lambda off, size: (w1[pl.ds(off, size), :], 1), 'n')
        else:
            send_partial(k, dhid.at[k], 3 * att_w, lambda off, size: (w2[:3 * att_w, pl.ds(off, size)], 0), 'n')
        if k == chunks - 1 and h + 1 < 2 * layers:
            load_weights(h + 1)

    def is_last(t):
        return t // chunks >= 2 * layers - 2

    def core_done(name, t):
        k = t % chunks
        _, kb, rb, xb, yb, i = bufs[name]
        flight[name, k][0].wait_recv()
        if is_last(t):
            flight[name, k][0].wait_send()
            sends[k] = [copy for copy in sends[k] if copy is not flight[name, k][0]]
        dt = kb.dtype
        for bx in (1, 0):
            for by in (1, 0):
                kb[k, bx, by] = (kb[k, bx, by].astype(F32) + rb[k, bx, by].astype(F32)).astype(dt)
        flight[name, k] = [remote(k, i + 1, kb.at[k, 1, :, :, cols_a], xb.at[k, :, :, cols_a], xax),
                           remote(k, i + 2, kb.at[k, :, 1, :, cols_b], xb.at[k, :, :, cols_b], yax)]

    def second_done(name, t):
        k = t % chunks
        _, kb, rb, xb, yb, i = bufs[name]
        dt = kb.dtype
        copy_a, copy_b = flight[name, k]
        copy_a.wait_recv()
        for j in (1, 0):
            kb[k, 0, j, :, :CUT] = (kb[k, 0, j, :, :CUT].astype(F32) + xb[k, j, :, :CUT].astype(F32)).astype(dt)
        third_a = remote(k, i + 3, kb.at[k, 0, 1, :, cols_a], yb.at[k, :, cols_a], yax)
        copy_b.wait_recv()
        for j in (1, 0):
            kb[k, j, 0, :, CUT:] = (kb[k, j, 0, :, CUT:].astype(F32) + xb[k, j, :, CUT:].astype(F32)).astype(dt)
        third_b = remote(k, i + 4, kb.at[k, 1, 0, :, cols_b], yb.at[k, :, cols_b], xax)
        flight[name, k] = [third_a, third_b]

    def quads(name, t):
        if is_last(t):
            return (s32, 10) if name == 'gn' else (r32, 15)
        return (quad_n, 10) if name == 'gn' else (quad_g, 15)

    def gather_start(name, t):
        k = t % chunks
        quad, i = quads(name, t)
        flight[name, k] = [
            remote(k, i, quad.at[k, 0, 0, :, cols_a], quad.at[k, 0, 1, :, cols_a], yax),
            remote(k, i + 1, quad.at[k, 0, 0, :, cols_b], quad.at[k, 1, 0, :, cols_b], xax)]

    def third_done(name, t):
        h, k = divmod(t, chunks)
        base, res, cot = (0, 1, 2) if h % 2 == 0 else (1, 0, 3)
        _, kb, rb, xb, yb, i = bufs[name]
        for copy in flight[name, k]:
            copy.wait_recv()
        summed = kb[k, 0, 0].astype(F32) + yb[k].astype(F32)
        for j in range(4):
            if ('own', j, k) in loads:
                loads.pop(('own', j, k)).wait()
        if name == 'f':
            value = own[res, k] - summed
            own[res, k] = value
            quad = quads('gn', t)[0]
            quad[k, 0, 0] = value if is_last(t) else rms_norm(value).astype(BF)
            gather_start('gn', t)
        else:
            x_in = own[base, k]
            inv = lax.rsqrt(jnp.mean(x_in * x_in, axis=-1, keepdims=True) + EPS)
            proj = jnp.mean(x_in * summed, axis=-1, keepdims=True)
            value = own[cot, k] + (inv * summed - x_in * (inv * inv * inv * proj))
            own[cot, k] = value
            quad = quads('gg', t)[0]
            quad[k, 0, 0] = value.astype(quad.dtype)
            gather_start('gg', t)

    def gather_second(name, t):
        k = t % chunks
        quad, i = quads(name, t)
        copy_a, copy_b = flight[name, k]
        copy_a.wait_recv()
        second_a = remote(k, i + 2, quad.at[k, 0, :, :, cols_a], quad.at[k, 1, :, :, cols_a], xax)
        copy_b.wait_recv()
        second_b = remote(k, i + 3, quad.at[k, :, 0, :, cols_b], quad.at[k, :, 1, :, cols_b], yax)
        flight[name, k] = [second_a, second_b]

    finals = []

    def gather_core(t):
        h, k = divmod(t, chunks)
        more = h + 1 < 2 * layers
        for name in ('gn', 'gg'):
            for copy in flight[name, k]:
                copy.wait_recv()
        if is_last(t):
            leaving = []
            outs = (x2, dx1) if h % 2 == 0 else (x1, dx2)
            for j, (name, out) in enumerate(zip(('gn', 'gg'), outs)):
                quad = quads(name, t)[0]
                for b in range(4):
                    bx, by = divmod(b, 2)
                    there = place(k, 0, bx, by)
                    far = pltpu.make_async_remote_copy(
                        src_ref=quad.at[k, bx, by], dst_ref=out.at[there], send_sem=fsend_sem.at[k, 4 * j + b],
                        recv_sem=frecv_sem.at[k, 4 * j + b], device_id=core, device_id_type=MESH)
                    far.start()
                    leaving.append((far, local(quad.at[k, bx, by], out.at[there], out_sem.at[k, 4 * j + b])))
            if more:
                for b in range(4):
                    bx, by = divmod(b, 2)
                    quad_n[k, bx, by] = rms_norm(s32[k, bx, by]).astype(BF)
                    quad_g[k, bx, by] = r32[k, bx, by].astype(BF)
                for far, near in leaving:
                    far.wait()
                    near.wait()
                for copy in sends[k]:
                    copy.wait_send()
                sends[k].clear()
            else:
                finals.extend(leaving)
        if more:
            arrivals['gn', k] = remote(k, 14, quad_n.at[k], next_n.at[k], core)
            arrivals['gg', k] = remote(k, 19, quad_g.at[k], next_g.at[k], core)

    def stage(slot, shape, dst):
        return pltpu.make_async_copy(aux.at[pl.ds(slot * 256, shape[0]), pl.ds(0, shape[1])], dst, wg_sem.at[slot])

    def weight_grads(h):
        layer = layers - 1 - h // 2
        mlp = h % 2 == 0
        total = chunks * rows

        def put(slot, value, dst, wait):
            copy = stage(slot, value.shape, dst)
            if wait is None:
                copy.wait()
            else:
                @pl.when(wait)
                def _():
                    copy.wait()
            aux[slot * 256:slot * 256 + value.shape[0], :value.shape[1]] = value
            copy.start()

        def wide(lhs, rhs, out, row0, lo, hi):
            def body(i, carry):
                off = pl.multiple_of(i * 256, 256)
                a = lhs[:, :, pl.ds(off, 256)].reshape(total, 256)
                for slot, (c0, cw) in enumerate(((0, CUT), (CUT, width - CUT))):
                    b = rhs[:, :, :, :, :, c0:c0 + cw].reshape(total, cw)
                    put(slot, dot(a, b, 0, 0), out.at[layer, pl.ds(row0 + off, 256), pl.ds(c0, cw)], i > lo)
                return carry
            lax.fori_loop(lo, hi, body, 0)
            for slot, (c0, cw) in enumerate(((0, CUT), (CUT, width - CUT))):
                stage(slot, (256, cw), out.at[layer, pl.ds(row0, 256), pl.ds(c0, cw)]).wait()

        def tall(lo, hi, size=256):
            cw = dhid.shape[-1] // 2

            def body(i, carry):
                off = i * 256 if size != 256 else pl.multiple_of(i * 256, 256)
                a = n_buf[:, :, :, :, :, pl.ds(off, size)].reshape(total, size)
                for slot in range(2):
                    b = dhid[:, :, slot * cw:(slot + 1) * cw].reshape(total, cw)
                    put(slot, dot(a, b, 0, 0), dwu.at[layer, pl.ds(off, size), pl.ds(slot * cw, cw)], i > lo)
                return carry
            if size == 256:
                lax.fori_loop(lo, hi, body, 0)
            else:
                body(lo, 0)
            for slot in range(2):
                stage(slot, (size, cw), dwu.at[layer, pl.ds(0, size), pl.ds(slot * cw, cw)]).wait()

        if not mlp:
            cut = 3 * att_w // 512
            return [lambda: wide(dhid, n_buf, dwa, 0, 0, cut), lambda: wide(dhid, n_buf, dwa, 0, cut, 3 * att_w // 256),
                    lambda: wide(hid, g_buf, dwa, 3 * att_w, 0, att_w // 256)]
        deep, high = hid.shape[-1] // 256, width // 256
        pieces = [lambda: wide(hid, g_buf, dwd, 0, 0, deep // 2), lambda: wide(hid, g_buf, dwd, 0, deep // 2, deep),
                  lambda: tall(0, high // 2), lambda: tall(high // 2, high)]
        if width % 256:
            pieces.append(lambda: tall(high, high, width % 256))
        return pieces

    tasks = 2 * layers * chunks
    for t in range(tasks + 2):
        pieces = []
        if t == 1:
            for i in range(2, len(firsts)):
                round_first(i)
        now, one_ago, two_ago = (0 <= i < tasks for i in (t, t - 1, t - 2))
        if now:
            compute(t)
            core_done('f', t)
            if t % chunks == chunks - 1:
                pieces = weight_grads(t // chunks)
        if one_ago:
            third_done('f', t - 1)
            third_done('n', t - 1)
        if now:
            compute_rest(t)
        if two_ago:
            gather_core(t - 2)
        if now:
            core_done('n', t)
        for piece in pieces[:1]:
            piece()
        if now:
            second_done('f', t)
        for piece in pieces[1:2]:
            piece()
        if now:
            second_done('n', t)
        if one_ago:
            gather_second('gn', t - 1)
            gather_second('gg', t - 1)
        for piece in pieces[2:]:
            piece()
    for far, near in finals:
        far.wait()
        near.wait()
    for k in range(chunks):
        for copy in sends[k]:
            copy.wait_send()


def run_stack(acts, w_att, w_up, w_down, heads, scale):
    layers, width, hid = w_up.shape
    att_w = w_att.shape[1] // 4
    seq = acts[0].shape[1]
    chunks = acts[0].shape[0] // GROUP
    rows = GROUP * seq
    quad = (chunks, 2, 2, seq, width)
    oct_ = (chunks, 2, 2, 2, seq, width)
    scratch = [pltpu.VMEM(oct_, BF), pltpu.VMEM(oct_, BF), pltpu.VMEM((width, hid), BF), pltpu.VMEM((hid, width), BF),
               pltpu.VMEM((4, chunks, seq, width), F32),
               pltpu.VMEM((chunks, rows, hid), BF), pltpu.VMEM((chunks, rows, hid), BF),
               pltpu.VMEM((rows, hid), F32)]
    for dt in (F32, BF):
        scratch += [pltpu.VMEM(quad, dt)] * 3
        scratch += [pltpu.VMEM((chunks, 2, seq, width), dt), pltpu.VMEM((chunks, seq, width), dt)]
    scratch += [pltpu.VMEM(quad, BF)] * 2
    dma = pltpu.SemaphoreType.DMA
    scratch += [dma((chunks, 4)), dma((2, 8)), dma((chunks, 4)), dma((2,)), dma((2,)), dma((chunks, 8)),
                dma((chunks, 20)), dma((chunks, 20)), dma((chunks, 8)), dma((chunks, 8))]
    any_spec = pl.BlockSpec(memory_space=pl.ANY)
    outs = [jax.ShapeDtypeStruct(a.shape, F32) for a in acts]
    outs += [jax.ShapeDtypeStruct(w.shape, F32) for w in (w_att, w_up, w_down)]
    outs += [jax.ShapeDtypeStruct(quad, BF)] * 2
    return pl.pallas_call(
        functools.partial(backward_pass, layers, chunks, seq, heads, att_w // heads, scale),
        out_shape=outs,
        in_specs=[any_spec] * 7,
        out_specs=[any_spec] * 9,
        scratch_shapes=scratch,
        compiler_params=pltpu.CompilerParams(collective_id=0, has_side_effects=True, vmem_limit_bytes=VMEM_LIMIT),
        name='backward_pass',
    )(*acts, w_att, w_up, w_down)


def copy_out(heads_att, head_dim, *refs):
    ins, outs = refs[:7], refs[7:]
    for src, dst in zip(ins[:6], outs[:6]):
        dst[...] = src[...]
    place = lax.rem(pl.program_id(0), heads_att)
    dq, do = outs[6:]

    @pl.when(place < 3 * heads_att // 4)
    def _():
        dq[...] = ins[6][:, :head_dim]

    @pl.when(place >= 3 * heads_att // 4)
    def _():
        do[...] = ins[6][:, :head_dim]


def write_results(acts, dwu, dwd, dwa, heads, head_dim):
    steps, seq, width = acts[0].shape
    layers = dwu.shape[0]
    per = steps // layers
    each = 4 * heads
    dwa = dwa.reshape(layers * each, -1, width)

    def split(a):
        return a.reshape(steps, -1, a.shape[-1])
    arrays = [*acts, split(dwu), split(dwd), dwa]

    def whole(a):
        return pl.BlockSpec((1,) + a.shape[1:], lambda i: (i, 0, 0))
    q_spec = pl.BlockSpec((1, head_dim, width), lambda i: (i // each * 3 * heads + jnp.minimum(i % each, 3 * heads - 1), 0, 0))
    o_spec = pl.BlockSpec((1, head_dim, width), lambda i: (i // each * heads + jnp.maximum(i % each - 3 * heads, 0), 0, 0))
    outs = pl.pallas_call(
        functools.partial(copy_out, each, head_dim),
        grid=(steps,),
        in_specs=[whole(a) for a in arrays],
        out_specs=[whole(a) for a in arrays[:6]] + [q_spec, o_spec],
        out_shape=[jax.ShapeDtypeStruct(a.shape, F32) for a in arrays[:6]] + [
            jax.ShapeDtypeStruct((layers * 3 * heads, head_dim, width), F32),
            jax.ShapeDtypeStruct((layers * heads, head_dim, width), F32)],
        compiler_params=pltpu.CompilerParams(vmem_limit_bytes=VMEM_LIMIT),
        name='write_results',
    )(*arrays)
    return (*outs[:4], outs[4].reshape(dwu.shape), outs[5].reshape(dwd.shape),
            outs[6].reshape(layers, 3, heads, head_dim, width), outs[7].reshape(layers, heads, head_dim, width))


def solution(mesh):
    act_spec = P('dp')
    in_specs = (act_spec, act_spec, act_spec, act_spec,
                P(None, None, None, 'tp', None), P(None, 'tp', None, None),
                P(None, None, 'tp'), P(None, 'tp', None))
    out_specs = (act_spec, act_spec, act_spec, act_spec,
                 P('dp', None, None, 'tp', None), P('dp', 'tp', None, None),
                 P('dp', None, 'tp'), P('dp', 'tp', None))

    def device_body(y_one, y_two, dy_one, dy_two, w_qkv, w_out, w_up, w_down):
        n_micro, n_batch, seq, width = y_one.shape
        layers, heads, head_dim = w_qkv.shape[0], w_qkv.shape[3], w_qkv.shape[4]
        pad = -head_dim % 128
        pdim = head_dim + pad
        chunks = n_micro * n_batch // GROUP
        acts = [a.reshape(chunks * GROUP, seq, width) for a in (y_one, y_two, dy_one, dy_two)]
        w_q = jnp.pad(w_qkv.transpose(0, 2, 3, 4, 1).reshape(layers, 3 * heads, head_dim, width), ((0, 0), (0, 0), (0, pad), (0, 0)))
        w_o = jnp.pad(w_out, ((0, 0), (0, 0), (0, pad), (0, 0)))
        w_att = jnp.concatenate([w_q, w_o], axis=1).reshape(layers, 4 * heads * pdim, width)
        x1, x2, dx1, dx2, dwa, dwu, dwd, _, _ = run_stack(acts, w_att, w_up, w_down, heads, head_dim ** -0.5)
        x1, x2, dx1, dx2, dwu, dwd, dwq, dwo = write_results((x1, x2, dx1, dx2), dwu, dwd, dwa, heads, head_dim)
        return (*(a.reshape(y_one.shape) for a in (x1, x2, dx1, dx2)), dwq.transpose(0, 4, 1, 2, 3), dwo, dwu, dwd)

    return jax.shard_map(device_body, mesh=mesh, in_specs=in_specs, out_specs=out_specs, check_vma=False)
```

```python
import functools

import jax
import jax.numpy as jnp
from jax import lax
from jax.experimental import pallas as pl
from jax.experimental.pallas import tpu as pltpu
from jax.sharding import PartitionSpec as P

EPS = 1e-6
BF = jnp.bfloat16
F32 = jnp.float32
GROUP = 8
CUT = 896
GELU_K = 0.7978845608028654
MESH = pl.DeviceIdType.MESH
VMEM_LIMIT = 67043328


def rms_norm(x_in):
    return x_in * lax.rsqrt(jnp.mean(x_in * x_in, axis=-1, keepdims=True) + EPS)


def dot(a, b, ca, cb):
    return lax.dot_general(a, b, (((ca,), (cb,)), ((), ())), preferred_element_type=F32)


def tiles(total, size, body):
    def step(i, carry):
        body(pl.multiple_of(i * size, size), size)
        return carry
    lax.fori_loop(0, total // size, step, 0)
    if total % size:
        body(total // size * size, total % size)


def backward_pass(layers, chunks, seq, heads, dim, scale, *refs):
    (y1, y2, dy1, dy2, wa_hbm, wu_hbm, wd_hbm,
     x1, x2, dx1, dx2, dwa, dwu, dwd, next_n, next_g,
     n_buf, g_buf, w1, w2, own, hid, dhid, aux, s32, k32, r32, x32, y32, s16, k16, r16, x16, y16,
     quad_n, quad_g, in_sem, first_sem, own_sem, w_sem, wg_sem, out_sem, send_sem, recv_sem, fsend_sem, frecv_sem) = refs
    width = n_buf.shape[-1]
    rows = GROUP * seq
    half = rows // 2
    att_w = heads * dim
    me = lax.axis_index('tp')
    my_core, my_x, my_y = lax.rem(me, 2), lax.rem(lax.div(me, 2), 2), lax.rem(lax.div(me, 4), 2)
    core, xax, yax = {'tp': me + 1 - 2 * my_core}, {'tp': me + 2 - 4 * my_x}, {'tp': me + 4 - 8 * my_y}

    barrier = pltpu.get_barrier_semaphore()
    for dev in (core, xax, yax):
        pl.semaphore_signal(barrier, inc=1, device_id=dev, device_id_type=MESH)

    def local(src, dst, sem):
        copy = pltpu.make_async_copy(src, dst, sem)
        copy.start()
        return copy

    loads = {}

    def load_weights(h):
        layer = layers - 1 - h // 2
        if h % 2 == 0:
            loads['w1'] = local(wu_hbm.at[layer], w1, w_sem.at[0])
            loads['w2'] = local(wd_hbm.at[layer], w2, w_sem.at[1])
        else:
            loads['w2'] = local(wa_hbm.at[layer], w2, w_sem.at[1])

    def place(k, c, bx, by):
        return k * GROUP + 4 * (my_core + c - 2 * c * my_core) + 2 * (my_x + bx - 2 * bx * my_x) + (
            my_y + by - 2 * by * my_y)

    firsts = [(k, src) for k in range(chunks) for src in (0, 1)]

    def fetch_first(i):
        k, src = firsts[i]
        slot = 1 + src
        loads['first', i] = [
            local((dy2 if src else y1).at[place(k, c, b // 2, b % 2)], (k32 if c else s32).at[slot, b // 2, b % 2],
                  first_sem.at[src, 4 * c + b]) for c in range(2) for b in range(4)]

    def round_first(i):
        k, src = firsts[i]
        slot = 1 + src
        for copy in loads.pop(('first', i)):
            copy.wait()
        for c in range(2):
            def one(b, carry):
                value = (k32 if c else s32)[slot, lax.div(b, 2), lax.rem(b, 2)]
                if src == 0:
                    n_buf[k, c, lax.div(b, 2), lax.rem(b, 2)] = rms_norm(value).astype(BF)
                else:
                    g_buf[k, c, lax.div(b, 2), lax.rem(b, 2)] = value.astype(BF)
                return carry
            lax.fori_loop(0, 4, one, 0)
        if i + 2 < len(firsts):
            fetch_first(i + 2)

    fetch_first(0)
    load_weights(0)
    fetch_first(1)
    mine = place(0, 0, 0, 0)
    for k in range(chunks):
        for j, src in enumerate((y1, y2, dy1, dy2)):
            loads['own', j, k] = local(src.at[k * GROUP + mine], own.at[j, k], own_sem.at[k, j])
    pl.semaphore_wait(barrier, 3)
    round_first(0)

    sends = [[] for _ in range(chunks)]
    flight, arrivals, staged = {}, {}, {}

    def remote(k, i, src, dst, dev):
        copy = pltpu.make_async_remote_copy(src_ref=src, dst_ref=dst, send_sem=send_sem.at[k, i],
                                            recv_sem=recv_sem.at[k, i], device_id=dev, device_id_type=MESH)
        copy.start()
        sends[k].append(copy)
        return copy

    def done_once(key):
        for copy in loads.pop(key, ()):
            copy.wait()

    cols_a, cols_b = pl.ds(0, CUT), pl.ds(CUT, width - CUT)
    bufs = {'f': (s32, k32, r32, x32, y32, 0), 'n': (s16, k16, r16, x16, y16, 5)}

    def send_partial(k, lhs, depth, weight, name):
        s_ref, k_ref, r_ref, _, _, i = bufs[name]

        def make(out, part):
            def tile(off, size):
                a = lhs[part * half:(part + 1) * half, :depth]
                b, cb = weight(off, size)
                out[k, :, :, :, pl.ds(off, size)] = dot(a, b, 1, cb).astype(out.dtype).reshape(2, 2, seq, size)
            tiles(width, 256, tile)
        make(s_ref, 1)
        flight[name, k] = [remote(k, i, s_ref.at[k], r_ref.at[k], core)]
        make(k_ref, 0)

    def chunk_of(buf, k):
        return buf[k].reshape(rows, width)

    def prefetch(t):
        h, k = divmod(t, chunks)
        if h > 0:
            for name, quad, nxt, buf, j in (('gn', quad_n, next_n, n_buf, 0), ('gg', quad_g, next_g, g_buf, 2)):
                first = local(quad.at[k], buf.at[k, 0], in_sem.at[k, j])
                arrivals.pop((name, k)).wait_recv()
                loads[name[1], k] = [first, local(nxt.at[k], buf.at[k, 1], in_sem.at[k, j + 1])]

    def compute(t):
        h, k = divmod(t, chunks)
        mlp = h % 2 == 0
        for copy in sends[k]:
            copy.wait_send()
        sends[k].clear()
        if k == 0:
            loads['w1' if mlp else 'w2'].wait()
        done_once(('n', k))
        if mlp:
            def up_tile(off, size):
                u = dot(chunk_of(n_buf, k), w1[:, pl.ds(off, size)], 1, 0)
                t_u = jnp.tanh(GELU_K * (u + 0.044715 * u * u * u))
                hid[k, :, pl.ds(off, size)] = (0.5 * u * (1.0 + t_u)).astype(BF)
                aux[:, pl.ds(off, size)] = 0.5 * (1.0 + t_u) + 0.5 * u * (1.0 - t_u * t_u) * (
                    GELU_K * (1.0 + 3 * 0.044715 * u * u))
            tiles(hid.shape[-1], 256, up_tile)
        else:
            def qkv_tile(off, size):
                hid[k, :, pl.ds(att_w + off, size)] = dot(chunk_of(n_buf, k), w2[pl.ds(off, size), :], 1, 1).astype(BF)
            tiles(3 * att_w, 256, qkv_tile)

            def fwd_seq(s, carry):
                r = pl.ds(pl.multiple_of(s * seq, seq), seq)
                for i in range(heads):
                    q, key, v = (hid[k, r, (j * heads + heads + i) * dim:(j * heads + heads + i + 1) * dim] for j in range(3))
                    scores = dot(q, key, 1, 1) * scale
                    expd = jnp.exp(scores - jnp.max(scores, axis=-1, keepdims=True))
                    prob = expd / jnp.sum(expd, axis=-1, keepdims=True)
                    aux[r, i * 128:i * 128 + seq] = prob
                    hid[k, r, i * dim:(i + 1) * dim] = dot(prob.astype(BF), v, 1, 0).astype(BF)
                return carry
            lax.fori_loop(0, GROUP, fwd_seq, 0, unroll=4)
        if k == 0 and mlp:
            loads['w2'].wait()
        row0, depth = (0, hid.shape[-1]) if mlp else (3 * att_w, att_w)
        send_partial(k, hid.at[k], depth, lambda off, size: (w2[row0:row0 + depth, pl.ds(off, size)], 0), 'f')
        if t == 0:
            round_first(1)
        done_once(('g', k))
        if mlp:
            def down_tile(off, size):
                d_act = dot(chunk_of(g_buf, k), w2[pl.ds(off, size), :], 1, 1)
                dhid[k, :, pl.ds(off, size)] = (d_act * aux[:, pl.ds(off, size)]).astype(BF)
            tiles(dhid.shape[-1], 256, down_tile)
        else:
            dhid[k, :, 3 * att_w:4 * att_w] = dot(chunk_of(g_buf, k), w2[3 * att_w:, :], 1, 1).astype(BF)

            def bwd_seq(s, carry):
                r = pl.ds(pl.multiple_of(s * seq, seq), seq)
                for i in range(heads):
                    q, key, v = (hid[k, r, (j * heads + heads + i) * dim:(j * heads + heads + i + 1) * dim] for j in range(3))
                    prob = aux[r, i * 128:i * 128 + seq]
                    d_out = dhid[k, r, 3 * att_w + i * dim:3 * att_w + (i + 1) * dim]
                    d_prob = dot(d_out, v, 1, 1).astype(BF).astype(F32)
                    row_dot = jnp.sum(d_prob * prob, axis=-1, keepdims=True)
                    d_score = (prob * (d_prob - row_dot) * scale).astype(BF)
                    parts = (dot(d_score, key, 1, 0), dot(d_score, q, 0, 0), dot(prob.astype(BF), d_out, 0, 0))
                    for j, part in enumerate(parts):
                        dhid[k, r, (j * heads + i) * dim:(j * heads + i + 1) * dim] = part.astype(BF)
                return carry
            lax.fori_loop(0, GROUP, bwd_seq, 0, unroll=4)

    def compute_rest(t):
        h, k = divmod(t, chunks)
        if h % 2 == 0:
            send_partial(k, dhid.at[k], dhid.shape[-1], lambda off, size: (w1[pl.ds(off, size), :], 1), 'n')
        else:
            send_partial(k, dhid.at[k], 3 * att_w, lambda off, size: (w2[:3 * att_w, pl.ds(off, size)], 0), 'n')
        if k == chunks - 1 and h + 1 < 2 * layers:
            load_weights(h + 1)

    def is_last(t):
        return t // chunks >= 2 * layers - 2

    def core_done(name, t):
        k = t % chunks
        _, kb, rb, xb, yb, i = bufs[name]
        flight[name, k][0].wait_recv()
        if is_last(t):
            flight[name, k][0].wait_send()
            sends[k] = [copy for copy in sends[k] if copy is not flight[name, k][0]]
        dt = kb.dtype
        for bx in (1, 0):
            for by in (1, 0):
                kb[k, bx, by] = (kb[k, bx, by].astype(F32) + rb[k, bx, by].astype(F32)).astype(dt)
        flight[name, k] = [remote(k, i + 1, kb.at[k, 1, :, :, cols_a], xb.at[k, :, :, cols_a], xax),
                           remote(k, i + 2, kb.at[k, :, 1, :, cols_b], xb.at[k, :, :, cols_b], yax)]

    def second_done(name, t):
        k = t % chunks
        _, kb, rb, xb, yb, i = bufs[name]
        dt = kb.dtype
        copy_a, copy_b = flight[name, k]
        copy_a.wait_recv()
        for j in (1, 0):
            kb[k, 0, j, :, :CUT] = (kb[k, 0, j, :, :CUT].astype(F32) + xb[k, j, :, :CUT].astype(F32)).astype(dt)
        third_a = remote(k, i + 3, kb.at[k, 0, 1, :, cols_a], yb.at[k, :, cols_a], yax)
        copy_b.wait_recv()
        for j in (1, 0):
            kb[k, j, 0, :, CUT:] = (kb[k, j, 0, :, CUT:].astype(F32) + xb[k, j, :, CUT:].astype(F32)).astype(dt)
        third_b = remote(k, i + 4, kb.at[k, 1, 0, :, cols_b], yb.at[k, :, cols_b], xax)
        flight[name, k] = [third_a, third_b]

    def quads(name, t):
        if is_last(t):
            return (s32, 10) if name == 'gn' else (r32, 15)
        return (quad_n, 10) if name == 'gn' else (quad_g, 15)

    def gather_start(name, t):
        k = t % chunks
        quad, i = quads(name, t)
        flight[name, k] = [
            remote(k, i, quad.at[k, 0, 0, :, cols_a], quad.at[k, 1, 0, :, cols_a], xax),
            remote(k, i + 1, quad.at[k, 0, 0, :, cols_b], quad.at[k, 0, 1, :, cols_b], yax)]

    def third_done(name, t):
        h, k = divmod(t, chunks)
        base, res, cot = (0, 1, 2) if h % 2 == 0 else (1, 0, 3)
        _, kb, rb, xb, yb, i = bufs[name]
        for copy in flight[name, k]:
            copy.wait_recv()
        summed = kb[k, 0, 0].astype(F32) + yb[k].astype(F32)
        for j in range(4):
            if ('own', j, k) in loads:
                loads.pop(('own', j, k)).wait()
        if name == 'f':
            value = own[res, k] - summed
            own[res, k] = value
            quad = quads('gn', t)[0]
            quad[k, 0, 0] = value if is_last(t) else rms_norm(value).astype(BF)
            gather_start('gn', t)
        else:
            x_in = own[base, k]
            inv = lax.rsqrt(jnp.mean(x_in * x_in, axis=-1, keepdims=True) + EPS)
            proj = jnp.mean(x_in * summed, axis=-1, keepdims=True)
            value = own[cot, k] + (inv * summed - x_in * (inv * inv * inv * proj))
            own[cot, k] = value
            quad = quads('gg', t)[0]
            quad[k, 0, 0] = value.astype(quad.dtype)
            gather_start('gg', t)

    def gather_second(name, t):
        k = t % chunks
        quad, i = quads(name, t)
        copy_a, copy_b = flight[name, k]
        copy_a.wait_recv()
        second_a = remote(k, i + 2, quad.at[k, :, 0, :, cols_a], quad.at[k, :, 1, :, cols_a], yax)
        copy_b.wait_recv()
        second_b = remote(k, i + 3, quad.at[k, 0, :, :, cols_b], quad.at[k, 1, :, :, cols_b], xax)
        flight[name, k] = [second_a, second_b]

    finals = []

    def gather_core(t):
        h, k = divmod(t, chunks)
        more = h + 1 < 2 * layers
        for name in ('gn', 'gg'):
            for copy in flight[name, k]:
                copy.wait_recv()
        if is_last(t):
            leaving = []
            outs = (x2, dx1) if h % 2 == 0 else (x1, dx2)
            for j, (name, out) in enumerate(zip(('gn', 'gg'), outs)):
                quad = quads(name, t)[0]
                for b in range(4):
                    bx, by = divmod(b, 2)
                    there = place(k, 0, bx, by)
                    far = pltpu.make_async_remote_copy(
                        src_ref=quad.at[k, bx, by], dst_ref=out.at[there], send_sem=fsend_sem.at[k, 4 * j + b],
                        recv_sem=frecv_sem.at[k, 4 * j + b], device_id=core, device_id_type=MESH)
                    far.start()
                    leaving.append((far, local(quad.at[k, bx, by], out.at[there], out_sem.at[k, 4 * j + b])))
            if more:
                for b in range(4):
                    bx, by = divmod(b, 2)
                    quad_n[k, bx, by] = rms_norm(s32[k, bx, by]).astype(BF)
                    quad_g[k, bx, by] = r32[k, bx, by].astype(BF)
                for far, near in leaving:
                    far.wait()
                    near.wait()
                for copy in sends[k]:
                    copy.wait_send()
                sends[k].clear()
            else:
                finals.extend(leaving)
        if more:
            arrivals['gn', k] = remote(k, 14, quad_n.at[k], next_n.at[k], core)
            arrivals['gg', k] = remote(k, 19, quad_g.at[k], next_g.at[k], core)

    def stage(slot, shape, dst):
        return pltpu.make_async_copy(aux.at[pl.ds(slot * 256, shape[0]), pl.ds(0, shape[1])], dst, wg_sem.at[slot])

    def weight_grads(h):
        layer = layers - 1 - h // 2
        mlp = h % 2 == 0
        total = chunks * rows

        def put(slot, value, dst, wait):
            copy = stage(slot, value.shape, dst)
            if wait is None:
                copy.wait()
            else:
                @pl.when(wait)
                def _():
                    copy.wait()
            aux[slot * 256:slot * 256 + value.shape[0], :value.shape[1]] = value
            copy.start()

        def wide(lhs, rhs, out, row0, lo, hi):
            def body(i, carry):
                off = pl.multiple_of(i * 256, 256)
                a = lhs[:, :, pl.ds(off, 256)].reshape(total, 256)
                for slot, (c0, cw) in enumerate(((0, CUT), (CUT, width - CUT))):
                    b = rhs[:, :, :, :, :, c0:c0 + cw].reshape(total, cw)
                    put(slot, dot(a, b, 0, 0), out.at[layer, pl.ds(row0 + off, 256), pl.ds(c0, cw)], i > lo)
                return carry
            lax.fori_loop(lo, hi, body, 0)
            for slot, (c0, cw) in enumerate(((0, CUT), (CUT, width - CUT))):
                stage(slot, (256, cw), out.at[layer, pl.ds(row0, 256), pl.ds(c0, cw)]).wait()

        def tall(lo, hi, size=256):
            cw = dhid.shape[-1] // 2

            def body(i, carry):
                off = i * 256 if size != 256 else pl.multiple_of(i * 256, 256)
                a = n_buf[:, :, :, :, :, pl.ds(off, size)].reshape(total, size)
                for slot in range(2):
                    b = dhid[:, :, slot * cw:(slot + 1) * cw].reshape(total, cw)
                    put(slot, dot(a, b, 0, 0), dwu.at[layer, pl.ds(off, size), pl.ds(slot * cw, cw)], i > lo)
                return carry
            if size == 256:
                lax.fori_loop(lo, hi, body, 0)
            else:
                body(lo, 0)
            for slot in range(2):
                stage(slot, (size, cw), dwu.at[layer, pl.ds(0, size), pl.ds(slot * cw, cw)]).wait()

        if not mlp:
            cut = 3 * att_w // 512
            return [lambda: wide(dhid, n_buf, dwa, 0, 0, cut), lambda: wide(dhid, n_buf, dwa, 0, cut, 3 * att_w // 256),
                    lambda: wide(hid, g_buf, dwa, 3 * att_w, 0, att_w // 256)]
        deep, high = hid.shape[-1] // 256, width // 256
        pieces = [lambda: wide(hid, g_buf, dwd, 0, 0, deep // 2), lambda: wide(hid, g_buf, dwd, 0, deep // 2, deep),
                  lambda: tall(0, high // 2), lambda: tall(high // 2, high)]
        if width % 256:
            pieces.append(lambda: tall(high, high, width % 256))
        return pieces

    tasks = 2 * layers * chunks
    early = set()
    for t in range(tasks + 2):
        pieces = []
        if t == 1:
            for i in range(2, len(firsts)):
                round_first(i)
        now, one_ago, two_ago = (0 <= i < tasks for i in (t, t - 1, t - 2))
        if now:
            compute(t)
            core_done('f', t)
            if t % chunks == chunks - 1:
                pieces = weight_grads(t // chunks)
        if one_ago and t - 1 not in early:
            third_done('f', t - 1)
            third_done('n', t - 1)
        if now:
            compute_rest(t)
        if two_ago:
            gather_core(t - 2)
        if now:
            core_done('n', t)
        for piece in pieces[:1]:
            piece()
        if now:
            second_done('f', t)
        for piece in pieces[1:2]:
            piece()
        if now:
            second_done('n', t)
        if t + 1 < tasks and not pieces:
            prefetch(t + 1)
        if one_ago:
            gather_second('gn', t - 1)
            gather_second('gg', t - 1)
        for piece in pieces[2:4]:
            piece()
        if len(pieces) > 4:
            third_done('f', t)
            third_done('n', t)
            early.add(t)
        for piece in pieces[4:]:
            piece()
        if t + 1 < tasks and pieces:
            prefetch(t + 1)
    for far, near in finals:
        far.wait()
        near.wait()
    for k in range(chunks):
        for copy in sends[k]:
            copy.wait_send()


def run_stack(acts, w_att, w_up, w_down, heads, scale):
    layers, width, hid = w_up.shape
    att_w = w_att.shape[1] // 4
    seq = acts[0].shape[1]
    chunks = acts[0].shape[0] // GROUP
    rows = GROUP * seq
    quad = (chunks, 2, 2, seq, width)
    oct_ = (chunks, 2, 2, 2, seq, width)
    scratch = [pltpu.VMEM(oct_, BF), pltpu.VMEM(oct_, BF), pltpu.VMEM((width, hid), BF), pltpu.VMEM((hid, width), BF),
               pltpu.VMEM((4, chunks, seq, width), F32),
               pltpu.VMEM((chunks, rows, hid), BF), pltpu.VMEM((chunks, rows, hid), BF),
               pltpu.VMEM((rows, hid), F32)]
    for dt in (F32, BF):
        scratch += [pltpu.VMEM(quad, dt)] * 3
        scratch += [pltpu.VMEM((chunks, 2, seq, width), dt), pltpu.VMEM((chunks, seq, width), dt)]
    scratch += [pltpu.VMEM(quad, BF)] * 2
    dma = pltpu.SemaphoreType.DMA
    scratch += [dma((chunks, 4)), dma((2, 8)), dma((chunks, 4)), dma((2,)), dma((2,)), dma((chunks, 8)),
                dma((chunks, 20)), dma((chunks, 20)), dma((chunks, 8)), dma((chunks, 8))]
    any_spec = pl.BlockSpec(memory_space=pl.ANY)
    outs = [jax.ShapeDtypeStruct(a.shape, F32) for a in acts]
    outs += [jax.ShapeDtypeStruct(w.shape, F32) for w in (w_att, w_up, w_down)]
    outs += [jax.ShapeDtypeStruct(quad, BF)] * 2
    return pl.pallas_call(
        functools.partial(backward_pass, layers, chunks, seq, heads, att_w // heads, scale),
        out_shape=outs,
        in_specs=[any_spec] * 7,
        out_specs=[any_spec] * 9,
        scratch_shapes=scratch,
        compiler_params=pltpu.CompilerParams(collective_id=0, has_side_effects=True, vmem_limit_bytes=VMEM_LIMIT),
        name='backward_pass',
    )(*acts, w_att, w_up, w_down)


def copy_out(heads_att, head_dim, *refs):
    ins, outs = refs[:7], refs[7:]
    for src, dst in zip(ins[:6], outs[:6]):
        dst[...] = src[...]
    place = lax.rem(pl.program_id(0), heads_att)
    dq, do = outs[6:]

    @pl.when(place < 3 * heads_att // 4)
    def _():
        dq[...] = ins[6][:, :head_dim]

    @pl.when(place >= 3 * heads_att // 4)
    def _():
        do[...] = ins[6][:, :head_dim]


def write_results(acts, dwu, dwd, dwa, heads, head_dim):
    steps, seq, width = acts[0].shape
    layers = dwu.shape[0]
    per = steps // layers
    each = 4 * heads
    dwa = dwa.reshape(layers * each, -1, width)

    def split(a):
        return a.reshape(steps, -1, a.shape[-1])
    arrays = [*acts, split(dwu), split(dwd), dwa]

    def whole(a):
        return pl.BlockSpec((1,) + a.shape[1:], lambda i: (i, 0, 0))
    q_spec = pl.BlockSpec((1, head_dim, width), lambda i: (i // each * 3 * heads + jnp.minimum(i % each, 3 * heads - 1), 0, 0))
    o_spec = pl.BlockSpec((1, head_dim, width), lambda i: (i // each * heads + jnp.maximum(i % each - 3 * heads, 0), 0, 0))
    outs = pl.pallas_call(
        functools.partial(copy_out, each, head_dim),
        grid=(steps,),
        in_specs=[whole(a) for a in arrays],
        out_specs=[whole(a) for a in arrays[:6]] + [q_spec, o_spec],
        out_shape=[jax.ShapeDtypeStruct(a.shape, F32) for a in arrays[:6]] + [
            jax.ShapeDtypeStruct((layers * 3 * heads, head_dim, width), F32),
            jax.ShapeDtypeStruct((layers * heads, head_dim, width), F32)],
        compiler_params=pltpu.CompilerParams(vmem_limit_bytes=VMEM_LIMIT),
        name='write_results',
    )(*arrays)
    return (*outs[:4], outs[4].reshape(dwu.shape), outs[5].reshape(dwd.shape),
            outs[6].reshape(layers, 3, heads, head_dim, width), outs[7].reshape(layers, heads, head_dim, width))


def solution(mesh):
    act_spec = P('dp')
    in_specs = (act_spec, act_spec, act_spec, act_spec,
                P(None, None, None, 'tp', None), P(None, 'tp', None, None),
                P(None, None, 'tp'), P(None, 'tp', None))
    out_specs = (act_spec, act_spec, act_spec, act_spec,
                 P('dp', None, None, 'tp', None), P('dp', 'tp', None, None),
                 P('dp', None, 'tp'), P('dp', 'tp', None))

    def device_body(y_one, y_two, dy_one, dy_two, w_qkv, w_out, w_up, w_down):
        n_micro, n_batch, seq, width = y_one.shape
        layers, heads, head_dim = w_qkv.shape[0], w_qkv.shape[3], w_qkv.shape[4]
        pad = -head_dim % 128
        pdim = head_dim + pad
        chunks = n_micro * n_batch // GROUP
        acts = [a.reshape(chunks * GROUP, seq, width) for a in (y_one, y_two, dy_one, dy_two)]
        w_q = jnp.pad(w_qkv.transpose(0, 2, 3, 4, 1).reshape(layers, 3 * heads, head_dim, width), ((0, 0), (0, 0), (0, pad), (0, 0)))
        w_o = jnp.pad(w_out, ((0, 0), (0, 0), (0, pad), (0, 0)))
        w_att = jnp.concatenate([w_q, w_o], axis=1).reshape(layers, 4 * heads * pdim, width)
        x1, x2, dx1, dx2, dwa, dwu, dwd, _, _ = run_stack(acts, w_att, w_up, w_down, heads, head_dim ** -0.5)
        x1, x2, dx1, dx2, dwu, dwd, dwq, dwo = write_results((x1, x2, dx1, dx2), dwu, dwd, dwa, heads, head_dim)
        return (*(a.reshape(y_one.shape) for a in (x1, x2, dx1, dx2)), dwq.transpose(0, 4, 1, 2, 3), dwo, dwu, dwd)

    return jax.shard_map(device_body, mesh=mesh, in_specs=in_specs, out_specs=out_specs, check_vma=False)
```

```python
import functools

import jax
import jax.numpy as jnp
from jax import lax
from jax.experimental import pallas as pl
from jax.experimental.pallas import tpu as pltpu
from jax.sharding import PartitionSpec as P

EPS = 1e-6
BF = jnp.bfloat16
F32 = jnp.float32
GROUP = 8
CUT = 896
GELU_K = 0.7978845608028654
MESH = pl.DeviceIdType.MESH
VMEM_LIMIT = 67043328


def rms_norm(x_in):
    return x_in * lax.rsqrt(jnp.mean(x_in * x_in, axis=-1, keepdims=True) + EPS)


def dot(a, b, ca, cb):
    return lax.dot_general(a, b, (((ca,), (cb,)), ((), ())), preferred_element_type=F32)


def tiles(total, size, body):
    def step(i, carry):
        body(pl.multiple_of(i * size, size), size)
        return carry
    lax.fori_loop(0, total // size, step, 0)
    if total % size:
        body(total // size * size, total % size)


def backward_pass(layers, chunks, seq, heads, dim, scale, *refs):
    (y1, y2, dy1, dy2, wa_hbm, wu_hbm, wd_hbm,
     x1, x2, dx1, dx2, dwa, dwu, dwd, next_n, next_g,
     n_buf, g_buf, w1, w2, own, hid, dhid, aux, s32, k32, r32, x32, y32, s16, k16, r16, x16, y16,
     quad_n, quad_g, in_sem, first_sem, own_sem, w_sem, wg_sem, out_sem, send_sem, recv_sem, fsend_sem, frecv_sem) = refs
    width = n_buf.shape[-1]
    rows = GROUP * seq
    half = rows // 2
    att_w = heads * dim
    me = lax.axis_index('tp')
    my_core, my_x, my_y = lax.rem(me, 2), lax.rem(lax.div(me, 2), 2), lax.rem(lax.div(me, 4), 2)
    core, xax, yax = {'tp': me + 1 - 2 * my_core}, {'tp': me + 2 - 4 * my_x}, {'tp': me + 4 - 8 * my_y}

    barrier = pltpu.get_barrier_semaphore()
    for dev in (core, xax, yax):
        pl.semaphore_signal(barrier, inc=1, device_id=dev, device_id_type=MESH)

    def local(src, dst, sem):
        copy = pltpu.make_async_copy(src, dst, sem)
        copy.start()
        return copy

    loads = {}

    def load_weights(h):
        layer = layers - 1 - h // 2
        if h % 2 == 0:
            loads['w1'] = local(wu_hbm.at[layer], w1, w_sem.at[0])
            loads['w2'] = local(wd_hbm.at[layer], w2, w_sem.at[1])
        else:
            loads['w2'] = local(wa_hbm.at[layer], w2, w_sem.at[1])

    def place(k, c, bx, by):
        return k * GROUP + 4 * (my_core + c - 2 * c * my_core) + 2 * (my_x + bx - 2 * bx * my_x) + (
            my_y + by - 2 * by * my_y)

    firsts = [(k, src) for k in range(chunks) for src in (0, 1)]

    def fetch_first(i):
        k, src = firsts[i]
        slot = 1 + src
        loads['first', i] = [
            local((dy2 if src else y1).at[place(k, c, b // 2, b % 2)], (k32 if c else s32).at[slot, b // 2, b % 2],
                  first_sem.at[src, 4 * c + b]) for c in range(2) for b in range(4)]

    def round_first(i):
        k, src = firsts[i]
        slot = 1 + src
        for copy in loads.pop(('first', i)):
            copy.wait()
        for c in range(2):
            def one(b, carry):
                value = (k32 if c else s32)[slot, lax.div(b, 2), lax.rem(b, 2)]
                if src == 0:
                    n_buf[k, c, lax.div(b, 2), lax.rem(b, 2)] = rms_norm(value).astype(BF)
                else:
                    g_buf[k, c, lax.div(b, 2), lax.rem(b, 2)] = value.astype(BF)
                return carry
            lax.fori_loop(0, 4, one, 0)
        if i + 2 < len(firsts):
            fetch_first(i + 2)

    fetch_first(0)
    load_weights(0)
    fetch_first(1)
    mine = place(0, 0, 0, 0)
    for k in range(chunks):
        for j, src in enumerate((y1, y2, dy1, dy2)):
            loads['own', j, k] = local(src.at[k * GROUP + mine], own.at[j, k], own_sem.at[k, j])
    pl.semaphore_wait(barrier, 3)
    round_first(0)

    sends = [[] for _ in range(chunks)]
    flight, arrivals, staged = {}, {}, {}

    def remote(k, i, src, dst, dev):
        copy = pltpu.make_async_remote_copy(src_ref=src, dst_ref=dst, send_sem=send_sem.at[k, i],
                                            recv_sem=recv_sem.at[k, i], device_id=dev, device_id_type=MESH)
        copy.start()
        sends[k].append(copy)
        return copy

    def done_once(key):
        for copy in loads.pop(key, ()):
            copy.wait()

    cols_a, cols_b = pl.ds(0, CUT), pl.ds(CUT, width - CUT)
    bufs = {'f': (s32, k32, r32, x32, y32, 0), 'n': (s16, k16, r16, x16, y16, 5)}

    def send_partial(k, lhs, depth, weight, name):
        s_ref, k_ref, r_ref, _, _, i = bufs[name]

        def make(out, part):
            def tile(off, size):
                a = lhs[part * half:(part + 1) * half, :depth]
                b, cb = weight(off, size)
                out[k, :, :, :, pl.ds(off, size)] = dot(a, b, 1, cb).astype(out.dtype).reshape(2, 2, seq, size)
            tiles(width, 256, tile)
        make(s_ref, 1)
        flight[name, k] = [remote(k, i, s_ref.at[k], r_ref.at[k], core)]
        make(k_ref, 0)

    def chunk_of(buf, k):
        return buf[k].reshape(rows, width)

    def prefetch(t):
        h, k = divmod(t, chunks)
        if h > 0:
            for name, quad, nxt, buf, j in (('gn', quad_n, next_n, n_buf, 0), ('gg', quad_g, next_g, g_buf, 2)):
                first = local(quad.at[k], buf.at[k, 0], in_sem.at[k, j])
                arrivals.pop((name, k)).wait_recv()
                loads[name[1], k] = [first, local(nxt.at[k], buf.at[k, 1], in_sem.at[k, j + 1])]

    def compute(t):
        h, k = divmod(t, chunks)
        mlp = h % 2 == 0
        for copy in sends[k]:
            copy.wait_send()
        sends[k].clear()
        if k == 0:
            loads['w1' if mlp else 'w2'].wait()
        done_once(('n', k))
        if mlp:
            def up_tile(off, size):
                u = dot(chunk_of(n_buf, k), w1[:, pl.ds(off, size)], 1, 0)
                t_u = jnp.tanh(GELU_K * (u + 0.044715 * u * u * u))
                hid[k, :, pl.ds(off, size)] = (0.5 * u * (1.0 + t_u)).astype(BF)
                aux[:, pl.ds(off, size)] = 0.5 * (1.0 + t_u) + 0.5 * u * (1.0 - t_u * t_u) * (
                    GELU_K * (1.0 + 3 * 0.044715 * u * u))
            tiles(hid.shape[-1], 256, up_tile)
        else:
            def qkv_tile(off, size):
                hid[k, :, pl.ds(att_w + off, size)] = dot(chunk_of(n_buf, k), w2[pl.ds(off, size), :], 1, 1).astype(BF)
            tiles(3 * att_w, 256, qkv_tile)

            def fwd_seq(s, carry):
                r = pl.ds(pl.multiple_of(s * seq, seq), seq)
                for i in range(heads):
                    q, key, v = (hid[k, r, (j * heads + heads + i) * dim:(j * heads + heads + i + 1) * dim] for j in range(3))
                    scores = dot(q, key, 1, 1) * scale
                    expd = jnp.exp(scores - jnp.max(scores, axis=-1, keepdims=True))
                    prob = expd / jnp.sum(expd, axis=-1, keepdims=True)
                    aux[r, i * 128:i * 128 + seq] = prob
                    hid[k, r, i * dim:(i + 1) * dim] = dot(prob.astype(BF), v, 1, 0).astype(BF)
                return carry
            lax.fori_loop(0, GROUP, fwd_seq, 0, unroll=4)
        if k == 0 and mlp:
            loads['w2'].wait()
        row0, depth = (0, hid.shape[-1]) if mlp else (3 * att_w, att_w)
        send_partial(k, hid.at[k], depth, lambda off, size: (w2[row0:row0 + depth, pl.ds(off, size)], 0), 'f')
        if t == 0:
            round_first(1)
        done_once(('g', k))
        if mlp:
            def down_tile(off, size):
                d_act = dot(chunk_of(g_buf, k), w2[pl.ds(off, size), :], 1, 1)
                dhid[k, :, pl.ds(off, size)] = (d_act * aux[:, pl.ds(off, size)]).astype(BF)
            tiles(dhid.shape[-1], 256, down_tile)
        else:
            dhid[k, :, 3 * att_w:4 * att_w] = dot(chunk_of(g_buf, k), w2[3 * att_w:, :], 1, 1).astype(BF)

            def bwd_seq(s, carry):
                r = pl.ds(pl.multiple_of(s * seq, seq), seq)
                for i in range(heads):
                    q, key, v = (hid[k, r, (j * heads + heads + i) * dim:(j * heads + heads + i + 1) * dim] for j in range(3))
                    prob = aux[r, i * 128:i * 128 + seq]
                    d_out = dhid[k, r, 3 * att_w + i * dim:3 * att_w + (i + 1) * dim]
                    d_prob = dot(d_out, v, 1, 1).astype(BF).astype(F32)
                    row_dot = jnp.sum(d_prob * prob, axis=-1, keepdims=True)
                    d_score = (prob * (d_prob - row_dot) * scale).astype(BF)
                    parts = (dot(d_score, key, 1, 0), dot(d_score, q, 0, 0), dot(prob.astype(BF), d_out, 0, 0))
                    for j, part in enumerate(parts):
                        dhid[k, r, (j * heads + i) * dim:(j * heads + i + 1) * dim] = part.astype(BF)
                return carry
            lax.fori_loop(0, GROUP, bwd_seq, 0, unroll=4)

    def compute_rest(t):
        h, k = divmod(t, chunks)
        if h % 2 == 0:
            send_partial(k, dhid.at[k], dhid.shape[-1], lambda off, size: (w1[pl.ds(off, size), :], 1), 'n')
        else:
            send_partial(k, dhid.at[k], 3 * att_w, lambda off, size: (w2[:3 * att_w, pl.ds(off, size)], 0), 'n')
        if k == chunks - 1 and h + 1 < 2 * layers:
            load_weights(h + 1)

    def is_last(t):
        return t // chunks >= 2 * layers - 2

    def core_done(name, t):
        k = t % chunks
        _, kb, rb, xb, yb, i = bufs[name]
        flight[name, k][0].wait_recv()
        if is_last(t):
            flight[name, k][0].wait_send()
            sends[k] = [copy for copy in sends[k] if copy is not flight[name, k][0]]
        dt = kb.dtype
        for bx in (1, 0):
            for by in (1, 0):
                kb[k, bx, by] = (kb[k, bx, by].astype(F32) + rb[k, bx, by].astype(F32)).astype(dt)
        flight[name, k] = [remote(k, i + 1, kb.at[k, 1, :, :, cols_a], xb.at[k, :, :, cols_a], xax),
                           remote(k, i + 2, kb.at[k, :, 1, :, cols_b], xb.at[k, :, :, cols_b], yax)]

    def second_done(name, t):
        k = t % chunks
        _, kb, rb, xb, yb, i = bufs[name]
        dt = kb.dtype
        copy_a, copy_b = flight[name, k]
        copy_a.wait_recv()
        for j in (1, 0):
            kb[k, 0, j, :, :CUT] = (kb[k, 0, j, :, :CUT].astype(F32) + xb[k, j, :, :CUT].astype(F32)).astype(dt)
        third_a = remote(k, i + 3, kb.at[k, 0, 1, :, cols_a], yb.at[k, :, cols_a], yax)
        copy_b.wait_recv()
        for j in (1, 0):
            kb[k, j, 0, :, CUT:] = (kb[k, j, 0, :, CUT:].astype(F32) + xb[k, j, :, CUT:].astype(F32)).astype(dt)
        third_b = remote(k, i + 4, kb.at[k, 1, 0, :, cols_b], yb.at[k, :, cols_b], xax)
        flight[name, k] = [third_a, third_b]

    def quads(name, t):
        if is_last(t):
            return (s32, 10) if name == 'gn' else (r32, 15)
        return (quad_n, 10) if name == 'gn' else (quad_g, 15)

    def gather_start(name, t):
        k = t % chunks
        quad, i = quads(name, t)
        flight[name, k] = [
            remote(k, i, quad.at[k, 0, 0, :, cols_a], quad.at[k, 1, 0, :, cols_a], xax),
            remote(k, i + 1, quad.at[k, 0, 0, :, cols_b], quad.at[k, 0, 1, :, cols_b], yax)]

    def third_done(name, t):
        h, k = divmod(t, chunks)
        base, res, cot = (0, 1, 2) if h % 2 == 0 else (1, 0, 3)
        _, kb, rb, xb, yb, i = bufs[name]
        for copy in flight[name, k]:
            copy.wait_recv()
        summed = kb[k, 0, 0].astype(F32) + yb[k].astype(F32)
        for j in range(4):
            if ('own', j, k) in loads:
                loads.pop(('own', j, k)).wait()
        if name == 'f':
            value = own[res, k] - summed
            own[res, k] = value
            quad = quads('gn', t)[0]
            quad[k, 0, 0] = value if is_last(t) else rms_norm(value).astype(BF)
            gather_start('gn', t)
        else:
            x_in = own[base, k]
            inv = lax.rsqrt(jnp.mean(x_in * x_in, axis=-1, keepdims=True) + EPS)
            proj = jnp.mean(x_in * summed, axis=-1, keepdims=True)
            value = own[cot, k] + (inv * summed - x_in * (inv * inv * inv * proj))
            own[cot, k] = value
            quad = quads('gg', t)[0]
            quad[k, 0, 0] = value.astype(quad.dtype)
            gather_start('gg', t)

    def gather_second(name, t):
        k = t % chunks
        quad, i = quads(name, t)
        copy_a, copy_b = flight[name, k]
        copy_a.wait_recv()
        second_a = remote(k, i + 2, quad.at[k, :, 0, :, cols_a], quad.at[k, :, 1, :, cols_a], yax)
        copy_b.wait_recv()
        second_b = remote(k, i + 3, quad.at[k, 0, :, :, cols_b], quad.at[k, 1, :, :, cols_b], xax)
        flight[name, k] = [second_a, second_b]

    finals = []

    def gather_core(t):
        h, k = divmod(t, chunks)
        more = h + 1 < 2 * layers
        for name in ('gn', 'gg'):
            for copy in flight[name, k]:
                copy.wait_recv()
        if is_last(t):
            leaving = []
            outs = (x2, dx1) if h % 2 == 0 else (x1, dx2)
            for j, (name, out) in enumerate(zip(('gn', 'gg'), outs)):
                quad = quads(name, t)[0]
                for b in range(4):
                    bx, by = divmod(b, 2)
                    there = place(k, 0, bx, by)
                    far = pltpu.make_async_remote_copy(
                        src_ref=quad.at[k, bx, by], dst_ref=out.at[there], send_sem=fsend_sem.at[k, 4 * j + b],
                        recv_sem=frecv_sem.at[k, 4 * j + b], device_id=core, device_id_type=MESH)
                    far.start()
                    leaving.append((far, local(quad.at[k, bx, by], out.at[there], out_sem.at[k, 4 * j + b])))
            if more:
                for b in range(4):
                    bx, by = divmod(b, 2)
                    quad_n[k, bx, by] = rms_norm(s32[k, bx, by]).astype(BF)
                    quad_g[k, bx, by] = r32[k, bx, by].astype(BF)
                for far, near in leaving:
                    far.wait()
                    near.wait()
                for copy in sends[k]:
                    copy.wait_send()
                sends[k].clear()
            else:
                finals.extend(leaving)
        if more:
            arrivals['gn', k] = remote(k, 14, quad_n.at[k], next_n.at[k], core)
            arrivals['gg', k] = remote(k, 19, quad_g.at[k], next_g.at[k], core)

    def stage(slot, shape, dst):
        return pltpu.make_async_copy(aux.at[pl.ds(slot * 256, shape[0]), pl.ds(0, shape[1])], dst, wg_sem.at[slot])

    def weight_grads(h):
        layer = layers - 1 - h // 2
        mlp = h % 2 == 0
        total = chunks * rows

        def put(slot, value, dst, wait):
            copy = stage(slot, value.shape, dst)
            if wait is None:
                copy.wait()
            else:
                @pl.when(wait)
                def _():
                    copy.wait()
            aux[slot * 256:slot * 256 + value.shape[0], :value.shape[1]] = value
            copy.start()

        def wide(lhs, rhs, out, row0, lo, hi):
            def body(i, carry):
                off = pl.multiple_of(i * 256, 256)
                a = lhs[:, :, pl.ds(off, 256)].reshape(total, 256)
                for slot, (c0, cw) in enumerate(((0, CUT), (CUT, width - CUT))):
                    b = rhs[:, :, :, :, :, c0:c0 + cw].reshape(total, cw)
                    put(slot, dot(a, b, 0, 0), out.at[layer, pl.ds(row0 + off, 256), pl.ds(c0, cw)], i > lo)
                return carry
            lax.fori_loop(lo, hi, body, 0)
            for slot, (c0, cw) in enumerate(((0, CUT), (CUT, width - CUT))):
                stage(slot, (256, cw), out.at[layer, pl.ds(row0, 256), pl.ds(c0, cw)]).wait()

        def tall(lo, hi, size=256):
            cw = dhid.shape[-1] // 2

            def body(i, carry):
                off = i * 256 if size != 256 else pl.multiple_of(i * 256, 256)
                a = n_buf[:, :, :, :, :, pl.ds(off, size)].reshape(total, size)
                for slot in range(2):
                    b = dhid[:, :, slot * cw:(slot + 1) * cw].reshape(total, cw)
                    put(slot, dot(a, b, 0, 0), dwu.at[layer, pl.ds(off, size), pl.ds(slot * cw, cw)], i > lo)
                return carry
            if size == 256:
                lax.fori_loop(lo, hi, body, 0)
            else:
                body(lo, 0)
            for slot in range(2):
                stage(slot, (size, cw), dwu.at[layer, pl.ds(0, size), pl.ds(slot * cw, cw)]).wait()

        if not mlp:
            cut = 3 * att_w // 512
            return [lambda: wide(dhid, n_buf, dwa, 0, 0, cut), lambda: wide(dhid, n_buf, dwa, 0, cut, 3 * att_w // 256),
                    lambda: wide(hid, g_buf, dwa, 3 * att_w, 0, att_w // 256)]
        deep, high = hid.shape[-1] // 256, width // 256
        pieces = [lambda: wide(hid, g_buf, dwd, 0, 0, deep // 2), lambda: wide(hid, g_buf, dwd, 0, deep // 2, deep),
                  lambda: tall(0, high // 2), lambda: tall(high // 2, high)]
        if width % 256:
            pieces.append(lambda: tall(high, high, width % 256))
        return pieces

    tasks = 2 * layers * chunks
    early = set()
    for t in range(tasks + 2):
        pieces = []
        if t == 1:
            for i in range(2, len(firsts)):
                round_first(i)
        now, one_ago, two_ago = (0 <= i < tasks for i in (t, t - 1, t - 2))
        if now:
            compute(t)
            core_done('f', t)
            if t % chunks == chunks - 1:
                pieces = weight_grads(t // chunks)
        if one_ago and t - 1 not in early:
            third_done('f', t - 1)
            third_done('n', t - 1)
        if now:
            compute_rest(t)
        if now:
            core_done('n', t)
        if two_ago:
            gather_core(t - 2)
        for piece in pieces[:1]:
            piece()
        if now:
            second_done('f', t)
        for piece in pieces[1:2]:
            piece()
        if one_ago:
            gather_second('gn', t - 1)
        if now:
            second_done('n', t)
        if one_ago:
            gather_second('gg', t - 1)
        if t + 1 < tasks and not pieces:
            prefetch(t + 1)
        for piece in pieces[2:4]:
            piece()
        if len(pieces) > 4:
            third_done('f', t)
            third_done('n', t)
            early.add(t)
        for piece in pieces[4:]:
            piece()
        if t + 1 < tasks and pieces:
            prefetch(t + 1)
    for far, near in finals:
        far.wait()
        near.wait()
    for k in range(chunks):
        for copy in sends[k]:
            copy.wait_send()


def run_stack(acts, w_att, w_up, w_down, heads, scale):
    layers, width, hid = w_up.shape
    att_w = w_att.shape[1] // 4
    seq = acts[0].shape[1]
    chunks = acts[0].shape[0] // GROUP
    rows = GROUP * seq
    quad = (chunks, 2, 2, seq, width)
    oct_ = (chunks, 2, 2, 2, seq, width)
    scratch = [pltpu.VMEM(oct_, BF), pltpu.VMEM(oct_, BF), pltpu.VMEM((width, hid), BF), pltpu.VMEM((hid, width), BF),
               pltpu.VMEM((4, chunks, seq, width), F32),
               pltpu.VMEM((chunks, rows, hid), BF), pltpu.VMEM((chunks, rows, hid), BF),
               pltpu.VMEM((rows, hid), F32)]
    for dt in (F32, BF):
        scratch += [pltpu.VMEM(quad, dt)] * 3
        scratch += [pltpu.VMEM((chunks, 2, seq, width), dt), pltpu.VMEM((chunks, seq, width), dt)]
    scratch += [pltpu.VMEM(quad, BF)] * 2
    dma = pltpu.SemaphoreType.DMA
    scratch += [dma((chunks, 4)), dma((2, 8)), dma((chunks, 4)), dma((2,)), dma((2,)), dma((chunks, 8)),
                dma((chunks, 20)), dma((chunks, 20)), dma((chunks, 8)), dma((chunks, 8))]
    any_spec = pl.BlockSpec(memory_space=pl.ANY)
    outs = [jax.ShapeDtypeStruct(a.shape, F32) for a in acts]
    outs += [jax.ShapeDtypeStruct(w.shape, F32) for w in (w_att, w_up, w_down)]
    outs += [jax.ShapeDtypeStruct(quad, BF)] * 2
    return pl.pallas_call(
        functools.partial(backward_pass, layers, chunks, seq, heads, att_w // heads, scale),
        out_shape=outs,
        in_specs=[any_spec] * 7,
        out_specs=[any_spec] * 9,
        scratch_shapes=scratch,
        compiler_params=pltpu.CompilerParams(collective_id=0, has_side_effects=True, vmem_limit_bytes=VMEM_LIMIT),
        name='backward_pass',
    )(*acts, w_att, w_up, w_down)


def copy_out(heads_att, head_dim, *refs):
    ins, outs = refs[:7], refs[7:]
    for src, dst in zip(ins[:6], outs[:6]):
        dst[...] = src[...]
    place = lax.rem(pl.program_id(0), heads_att)
    dq, do = outs[6:]

    @pl.when(place < 3 * heads_att // 4)
    def _():
        dq[...] = ins[6][:, :head_dim]

    @pl.when(place >= 3 * heads_att // 4)
    def _():
        do[...] = ins[6][:, :head_dim]


def write_results(acts, dwu, dwd, dwa, heads, head_dim):
    steps, seq, width = acts[0].shape
    layers = dwu.shape[0]
    per = steps // layers
    each = 4 * heads
    dwa = dwa.reshape(layers * each, -1, width)

    def split(a):
        return a.reshape(steps, -1, a.shape[-1])
    arrays = [*acts, split(dwu), split(dwd), dwa]

    def whole(a):
        return pl.BlockSpec((1,) + a.shape[1:], lambda i: (i, 0, 0))
    q_spec = pl.BlockSpec((1, head_dim, width), lambda i: (i // each * 3 * heads + jnp.minimum(i % each, 3 * heads - 1), 0, 0))
    o_spec = pl.BlockSpec((1, head_dim, width), lambda i: (i // each * heads + jnp.maximum(i % each - 3 * heads, 0), 0, 0))
    outs = pl.pallas_call(
        functools.partial(copy_out, each, head_dim),
        grid=(steps,),
        in_specs=[whole(a) for a in arrays],
        out_specs=[whole(a) for a in arrays[:6]] + [q_spec, o_spec],
        out_shape=[jax.ShapeDtypeStruct(a.shape, F32) for a in arrays[:6]] + [
            jax.ShapeDtypeStruct((layers * 3 * heads, head_dim, width), F32),
            jax.ShapeDtypeStruct((layers * heads, head_dim, width), F32)],
        compiler_params=pltpu.CompilerParams(vmem_limit_bytes=VMEM_LIMIT),
        name='write_results',
    )(*arrays)
    return (*outs[:4], outs[4].reshape(dwu.shape), outs[5].reshape(dwd.shape),
            outs[6].reshape(layers, 3, heads, head_dim, width), outs[7].reshape(layers, heads, head_dim, width))


def solution(mesh):
    act_spec = P('dp')
    in_specs = (act_spec, act_spec, act_spec, act_spec,
                P(None, None, None, 'tp', None), P(None, 'tp', None, None),
                P(None, None, 'tp'), P(None, 'tp', None))
    out_specs = (act_spec, act_spec, act_spec, act_spec,
                 P('dp', None, None, 'tp', None), P('dp', 'tp', None, None),
                 P('dp', None, 'tp'), P('dp', 'tp', None))

    def device_body(y_one, y_two, dy_one, dy_two, w_qkv, w_out, w_up, w_down):
        n_micro, n_batch, seq, width = y_one.shape
        layers, heads, head_dim = w_qkv.shape[0], w_qkv.shape[3], w_qkv.shape[4]
        pad = -head_dim % 128
        pdim = head_dim + pad
        chunks = n_micro * n_batch // GROUP
        acts = [a.reshape(chunks * GROUP, seq, width) for a in (y_one, y_two, dy_one, dy_two)]
        w_q = jnp.pad(w_qkv.transpose(0, 2, 3, 4, 1).reshape(layers, 3 * heads, head_dim, width), ((0, 0), (0, 0), (0, pad), (0, 0)))
        w_o = jnp.pad(w_out, ((0, 0), (0, 0), (0, pad), (0, 0)))
        w_att = jnp.concatenate([w_q, w_o], axis=1).reshape(layers, 4 * heads * pdim, width)
        x1, x2, dx1, dx2, dwa, dwu, dwd, _, _ = run_stack(acts, w_att, w_up, w_down, heads, head_dim ** -0.5)
        x1, x2, dx1, dx2, dwu, dwd, dwq, dwo = write_results((x1, x2, dx1, dx2), dwu, dwd, dwa, heads, head_dim)
        return (*(a.reshape(y_one.shape) for a in (x1, x2, dx1, dx2)), dwq.transpose(0, 4, 1, 2, 3), dwo, dwu, dwd)

    return jax.shard_map(device_body, mesh=mesh, in_specs=in_specs, out_specs=out_specs, check_vma=False)
```
